128 devices in a mesh: dp: 16 (over y_hi, z, core), mp: 8 (over y_lo, x).
Axes of the slice: x: 4, y: 4 (y_hi: 2, y_lo: 2; y = y_hi * 2 + y_lo), z: 4, core: 2. Of those that a mesh axis runs over, the one named last changes fastest.
Arguments:
- features: bfloat16 [16384, 8192], P('dp', 'mp'), may hold values from -6 to 6
- v_weight: bfloat16 [3, 8192, 1024], P(None, 'mp', 'dp'), may hold values from -0.0625 to 0.0625
- u_weight: bfloat16 [3, 1024, 8192], P(None, 'dp', 'mp'), may hold values from -0.1875 to 0.1875
- cross_bias: float32 [3, 8192], P(None, 'mp'), may hold values from -3 to 3
Outputs:
- crossed: bfloat16 [16384, 8192], P('dp', 'mp')
The draws below stay inside these ranges and needn't reach their ends.
All inputs are finite; a program needn't handle non-finite values.
Results may differ from the reference program's by a relative error of at most 0.009.
Values may be sent and summed in bfloat16 or wider, within the bound.
A program may use at most 64 MiB of HBM per device.

```python
import jax
import jax.numpy as jnp

D = 8192
R = 1024
LAYERS = 3
BATCH = 16384


def block_levels(key, extent, split, low, top_value):
    factor_of = 1.0
    for axis_at, blocks in split:
        draws = jax.random.uniform(jax.random.fold_in(jax.random.fold_in(key, 6), axis_at), (blocks,), jnp.float32, low / len(split), top_value / len(split))
        factor_of = factor_of * jnp.repeat(jnp.exp(draws), extent[axis_at] // blocks).reshape((-1,) + (1,) * (len(extent) - 1 - axis_at))
    return factor_of


def scatter_about(key, shape, width, reach, shards=(), kind=jnp.bfloat16):
    entries = jax.random.normal(key, shape, jnp.float32) * width
    if len(shards) > 0:
        entries = block_levels(key, shape, shards, -0.22, 0.18) * entries
    return jnp.clip(entries, min=-reach, max=reach).astype(kind)


def setup_inputs(seed: int = 0) -> dict:
    key_of = jax.random.split(jax.random.key(seed), 5)
    features = scatter_about(key_of[0], (BATCH, D), 1.0, 6.0, ((0, 16), (1, 8)))
    v_weight = scatter_about(key_of[1], (LAYERS, D, R), D ** -0.5, 0.0625, ((1, 8), (2, 16)))
    u_weight = scatter_about(key_of[2], (LAYERS, R, D), R ** -0.5, 0.1875, ((1, 16), (2, 8)))
    cross_bias = scatter_about(key_of[3], (LAYERS, D), 0.5, 3.0, ((1, 8),), jnp.float32)
    return {"features": features, "v_weight": v_weight, "u_weight": u_weight, "cross_bias": cross_bias}


def reference(features, v_weight, u_weight, cross_bias):
    carried = features
    for layer_number in range(LAYERS):
        rank_proj = jnp.dot(carried, v_weight[layer_number], preferred_element_type=jnp.float32).astype(jnp.bfloat16)
        cross_term = jnp.dot(rank_proj, u_weight[layer_number], preferred_element_type=jnp.float32) + cross_bias[layer_number]
        carried = (features.astype(jnp.float32) * cross_term + carried.astype(jnp.float32)).astype(jnp.bfloat16)
    return carried
```

```python
import jax
import jax.numpy as jnp
from jax import lax
from jax.experimental import pallas as pl
from jax.experimental.pallas import tpu as pltpu
from jax.sharding import PartitionSpec as P

MESH = pl.DeviceIdType.MESH
BF16 = jnp.bfloat16
F32 = jnp.float32

CHUNKS = 8
LAG = (0, 1, 2, 3, 4, 5)


def kernel(
    f_ref, v_ref, u_ref, b_ref, out_ref,
    vbuf, v_full, u_full, carried, part, rank, rs1, s2, rs2, ysend, yrecv,
    ss, rs, wss, wrs, w0s, w0r,
):
    layers = v_ref.shape[0]
    rows = f_ref.shape[0] // CHUNKS
    half = rows // 2
    depth = f_ref.shape[1]
    feat_half = depth // 2
    share = u_ref.shape[1]
    block_width = 2 * share
    tasks = layers * CHUNKS
    quarter = v_full.shape[2] // 4

    dp, mp = lax.axis_index("dp"), lax.axis_index("mp")
    y_hi, z, core = dp // 8, lax.rem(dp // 2, 4), lax.rem(dp, 2)
    y_lo, x = mp // 4, lax.rem(mp, 4)
    xr, xl, xo = lax.rem(x + 1, 4), lax.rem(x + 3, 4), lax.rem(x + 2, 4)
    zr, zl, zo = lax.rem(z + 1, 4), lax.rem(z + 3, 4), lax.rem(z + 2, 4)

    def at(y_hi=y_hi, z=z, core=core, y_lo=y_lo, x=x):
        return ((y_hi * 4 + z) * 2 + core, y_lo * 4 + x)

    right, left, across = at(x=xr), at(x=xl), at(y_lo=1 - y_lo)
    z_right, z_left, y_far, partner = at(z=zr), at(z=zl), at(y_hi=1 - y_hi), at(core=1 - core)

    barrier = pltpu.get_barrier_semaphore()
    for device in (right, left, across, z_right, z_left, y_far, partner):
        pl.semaphore_signal(barrier, inc=1, device_id=device, device_id_type=MESH)
    pl.semaphore_wait(barrier, 7)

    def send(src, dst, send_sem, recv_sem, device):
        return pltpu.make_async_remote_copy(
            src_ref=src, dst_ref=dst, send_sem=send_sem, recv_sem=recv_sem,
            device_id=device, device_id_type=MESH,
        )

    own = y_hi * 4 + z
    same = y_hi * 4
    other = (1 - y_hi) * 4

    def piece(matrix, block):
        layer = matrix // 2
        if matrix % 2 == 0:
            return v_full.at[
                layer,
                pl.ds(pl.multiple_of(core * feat_half, feat_half), feat_half),
                pl.ds(pl.multiple_of(block * block_width, block_width), block_width),
            ]
        return u_full.at[layer, pl.ds(pl.multiple_of(block * block_width + core * share, share), share), :]

    def move(matrix, block, number, device):
        ref = piece(matrix, block)
        return send(ref, ref, wss.at[matrix, number], wrs.at[matrix, number], device)

    def swap_v(layer):
        return send(v_ref.at[layer], vbuf.at[layer], w0s.at[layer], w0r.at[layer], partner)

    def swap_u(layer):
        place = u_full.at[layer, pl.ds(pl.multiple_of(own * block_width + core * share, share), share), :]
        return send(u_ref.at[layer], place, w0s.at[layers + layer], w0r.at[layers + layer], partner)

    def far(matrix):
        return [move(matrix, own, 0, y_far), move(matrix, own, 1, z_right), move(matrix, own, 2, z_left)]

    def near(matrix):
        block = other + z
        return [move(matrix, block, 3, z_right), move(matrix, block, 4, z_left), move(matrix, block, 7, partner)]

    def onward(matrix):
        return [
            move(matrix, same + zl, 5, z_right),
            move(matrix, other + zr, 6, z_left),
            move(matrix, same + zl, 8, partner),
            move(matrix, same + zr, 9, partner),
            move(matrix, other + zl, 10, partner),
            move(matrix, other + zr, 11, partner),
        ]

    def last(matrix):
        return [move(matrix, same + zo, 12, partner), move(matrix, other + zo, 13, partner)]

    def arrived(matrix, numbers):
        for number in numbers:
            move(matrix, own, number, partner).wait_recv()

    def start(copies):
        for copy in copies:
            copy.start()

    def weights_0(matrix):
        layer = matrix // 2
        if matrix % 2 == 0:
            swap_v(layer).wait_recv()
            mine, theirs = v_ref[layer], vbuf[layer]
            first = core == 0
            low = jnp.where(first, mine, theirs)
            high = jnp.where(first, theirs, mine)
            v_full[layer, :, pl.ds(pl.multiple_of(own * block_width, block_width), block_width)] = (
                jnp.concatenate([low, high], axis=1)
            )
        start(far(matrix))

    def weights_1(matrix):
        arrived(matrix, (0,))
        start(near(matrix))

    def weights_2(matrix):
        arrived(matrix, (1, 2, 3, 4))
        start(onward(matrix))

    def weights_3(matrix):
        arrived(matrix, (5, 6))
        start(last(matrix))

    def weights_4(matrix):
        arrived(matrix, (7, 8, 9, 10, 11, 12, 13))
        if matrix % 2 == 1:
            swap_u(matrix // 2).wait_recv()

    weight_stages = (weights_0, weights_1, weights_2, weights_3, weights_4)

    upper, lower = pl.ds(0, half), pl.ds(half, half)

    def first_hop(t):
        return [
            send(part.at[t, xo, upper], rs1.at[t, 0], ss.at[t, 0], rs.at[t, 0], right),
            send(part.at[t, xo, lower], rs1.at[t, 2], ss.at[t, 2], rs.at[t, 2], left),
            send(part.at[t, xr, lower], rs1.at[t, 1], ss.at[t, 1], rs.at[t, 1], right),
            send(part.at[t, xl, upper], rs1.at[t, 3], ss.at[t, 3], rs.at[t, 3], left),
        ]

    def second_hop(t):
        return [
            send(s2.at[t, 0], rs2.at[t, 0], ss.at[t, 4], rs.at[t, 4], right),
            send(s2.at[t, 1], rs2.at[t, 1], ss.at[t, 5], rs.at[t, 5], left),
        ]

    def exchange(t):
        return [send(ysend.at[t], yrecv.at[t], ss.at[t, 6], rs.at[t, 6], across)]

    def share_1(t):
        return [
            send(rank.at[t, x], rank.at[t, x], ss.at[t, 7], rs.at[t, 7], right),
            send(rank.at[t, x], rank.at[t, x], ss.at[t, 8], rs.at[t, 8], left),
        ]

    def share_2(t):
        return [
            send(rank.at[t, xl, upper], rank.at[t, xl, upper], ss.at[t, 9], rs.at[t, 9], right),
            send(rank.at[t, xr, lower], rank.at[t, xr, lower], ss.at[t, 10], rs.at[t, 10], left),
        ]

    def stage_0(t):
        layer, chunk = t // CHUNKS, lax.rem(t, CHUNKS)
        for q in range(4):
            part[t, q] = jnp.dot(
                carried[chunk], v_full[layer, :, q * quarter : (q + 1) * quarter], preferred_element_type=F32
            ).astype(BF16)
        start(first_hop(t))

    def stage_1(t):
        hop = first_hop(t)
        hop[0].wait_recv()
        s2[t, 0] = (part[t, xr, upper].astype(F32) + rs1[t, 0].astype(F32)).astype(BF16)
        hop[1].wait_recv()
        s2[t, 1] = (part[t, xl, lower].astype(F32) + rs1[t, 2].astype(F32)).astype(BF16)
        start(second_hop(t))

    def stage_2(t):
        hop = first_hop(t)
        hop[2].wait_recv()
        hop[3].wait_recv()
        for copy in second_hop(t):
            copy.wait_recv()
        ysend[t, upper] = (
            part[t, x, upper].astype(F32) + rs2[t, 0].astype(F32) + rs1[t, 3].astype(F32)
        ).astype(BF16)
        ysend[t, lower] = (
            part[t, x, lower].astype(F32) + rs2[t, 1].astype(F32) + rs1[t, 1].astype(F32)
        ).astype(BF16)
        start(exchange(t))

    def stage_3(t):
        exchange(t)[0].wait_recv()
        rank[t, x] = (ysend[t].astype(F32) + yrecv[t].astype(F32)).astype(BF16)
        start(share_1(t))

    def stage_4(t):
        for copy in share_1(t):
            copy.wait_recv()
        start(share_2(t))

    def stage_5(t):
        layer, chunk = t // CHUNKS, lax.rem(t, CHUNKS)
        for copy in share_2(t):
            copy.wait_recv()
        where = pl.ds(pl.multiple_of(chunk * rows, rows), rows)
        for j in range(4):
            columns = slice(j * depth // 4, (j + 1) * depth // 4)
            total = b_ref[layer][:, columns]
            for q in range(4):
                total = total + jnp.dot(
                    rank[t, q],
                    u_full[layer, q * quarter : (q + 1) * quarter, columns],
                    preferred_element_type=F32,
                )
            carried[chunk, :, columns] = (
                f_ref[where, columns].astype(F32) * total + carried[chunk, :, columns].astype(F32)
            ).astype(BF16)

        @pl.when(layer == layers - 1)
        def _():
            out_ref[where, :] = carried[chunk]

    for layer in range(layers):
        swap_v(layer).start()
    for layer in range(layers):
        swap_u(layer).start()
    for layer in range(layers):
        u_full[layer, pl.ds(pl.multiple_of(own * block_width + core * share, share), share), :] = u_ref[layer]
    weights_0(0)

    @pl.loop(0, CHUNKS)
    def _(chunk):
        carried[chunk] = f_ref[pl.ds(pl.multiple_of(chunk * rows, rows), rows), :]

    weights_1(0)
    weights_2(0)
    weights_3(0)
    weights_0(1)
    weights_1(1)
    weights_4(0)

    plan = {}
    for stage in range(2, 5):
        plan.setdefault(stage - 2, []).append((stage, 1))
    for matrix, begin in ((2, 2), (3, 6), (4, 9), (5, 13)):
        for stage in range(5):
            plan.setdefault(begin + stage, []).append((stage, matrix))

    @pl.loop(0, tasks + LAG[5])
    def _(i):
        for when, steps in sorted(plan.items()):
            @pl.when(i == when)
            def _(steps=steps):
                for stage, matrix in steps:
                    weight_stages[stage](matrix)

        for number, stage in ((4, stage_4), (3, stage_3), (2, stage_2), (1, stage_1), (5, stage_5), (0, stage_0)):
            t = i - LAG[number]

            @pl.when(jnp.logical_and(t >= 0, t < tasks))
            def _(stage=stage, t=t):
                stage(t)

    @pl.loop(0, tasks)
    def _(t):
        for copies in (first_hop, second_hop, exchange, share_1, share_2):
            for copy in copies(t):
                copy.wait_send()

    for layer in range(layers):
        swap_v(layer).wait_send()
        swap_u(layer).wait_send()
    for matrix in range(2 * layers):
        for copies in (far, near, onward, last):
            for copy in copies(matrix):
                copy.wait_send()


def local(features, v_weight, u_weight, cross_bias):
    layers, depth, share = v_weight.shape
    rank = share * lax.axis_size("dp")
    rows = features.shape[0] // CHUNKS
    half = rows // 2
    quarter = rank // 4
    tasks = layers * CHUNKS
    dma = pltpu.SemaphoreType.DMA
    vmem = pl.BlockSpec(memory_space=pltpu.VMEM)
    return pl.pallas_call(
        kernel,
        out_shape=jax.ShapeDtypeStruct(features.shape, BF16),
        in_specs=[vmem] * 4,
        out_specs=vmem,
        scratch_shapes=[
            pltpu.VMEM((layers, depth, share), BF16),
            pltpu.VMEM((layers, depth, rank), BF16),
            pltpu.VMEM((layers, rank, depth), BF16),
            pltpu.VMEM((CHUNKS, rows, depth), BF16),
            pltpu.VMEM((tasks, 4, rows, quarter), BF16),
            pltpu.VMEM((tasks, 4, rows, quarter), BF16),
            pltpu.VMEM((tasks, 4, half, quarter), BF16),
            pltpu.VMEM((tasks, 2, half, quarter), BF16),
            pltpu.VMEM((tasks, 2, half, quarter), BF16),
            pltpu.VMEM((tasks, rows, quarter), BF16),
            pltpu.VMEM((tasks, rows, quarter), BF16),
            dma((tasks, 11)),
            dma((tasks, 11)),
            dma((2 * layers, 14)),
            dma((2 * layers, 14)),
            dma((2 * layers,)),
            dma((2 * layers,)),
        ],
        compiler_params=pltpu.CompilerParams(
            collective_id=0, has_side_effects=True, vmem_limit_bytes=67043328
        ),
    )(features, v_weight, u_weight, cross_bias.reshape(layers, 1, depth))


def solution(mesh):
    return jax.shard_map(
        local,
        mesh=mesh,
        in_specs=(P("dp", "mp"), P(None, "mp", "dp"), P(None, "dp", "mp"), P(None, "mp")),
        out_specs=P("dp", "mp"),
        check_vma=False,
    )
```

```python
import jax
import jax.numpy as jnp
from jax import lax
from jax.experimental import pallas as pl
from jax.experimental.pallas import tpu as pltpu
from jax.sharding import PartitionSpec as P

MESH = pl.DeviceIdType.MESH
BF16 = jnp.bfloat16
F32 = jnp.float32

CHUNKS = 8
LAG = (0, 1, 2, 3, 4, 5)


def kernel(
    f_ref, v_ref, u_ref, b_ref, out_ref,
    w_full, carried, part, rank, rs1, s2, rs2, ysend, yrecv,
    ss, rs, wss, wrs,
):
    layers = v_ref.shape[0]
    rows = f_ref.shape[0] // CHUNKS
    half = rows // 2
    depth = f_ref.shape[1]
    share = u_ref.shape[1]
    block_width = 2 * share
    tasks = layers * CHUNKS
    quarter = w_full.shape[1] // 4

    dp, mp = lax.axis_index("dp"), lax.axis_index("mp")
    y_hi, z, core = dp // 8, lax.rem(dp // 2, 4), lax.rem(dp, 2)
    y_lo, x = mp // 4, lax.rem(mp, 4)
    xr, xl, xo = lax.rem(x + 1, 4), lax.rem(x + 3, 4), lax.rem(x + 2, 4)
    zr, zl, zo = lax.rem(z + 1, 4), lax.rem(z + 3, 4), lax.rem(z + 2, 4)

    def at(y_hi=y_hi, z=z, core=core, y_lo=y_lo, x=x):
        return ((y_hi * 4 + z) * 2 + core, y_lo * 4 + x)

    right, left, across = at(x=xr), at(x=xl), at(y_lo=1 - y_lo)
    z_right, z_left, y_far, partner = at(z=zr), at(z=zl), at(y_hi=1 - y_hi), at(core=1 - core)

    barrier = pltpu.get_barrier_semaphore()
    for device in (right, left, across, z_right, z_left, y_far, partner):
        pl.semaphore_signal(barrier, inc=1, device_id=device, device_id_type=MESH)
    pl.semaphore_wait(barrier, 7)

    def send(src, dst, send_sem, recv_sem, device):
        return pltpu.make_async_remote_copy(
            src_ref=src, dst_ref=dst, send_sem=send_sem, recv_sem=recv_sem,
            device_id=device, device_id_type=MESH,
        )

    own = y_hi * 4 + z
    same = y_hi * 4
    other = (1 - y_hi) * 4

    def piece(matrix, block):
        first = pl.multiple_of(block * block_width + core * share, share)
        return w_full.at[matrix, pl.ds(first, share), :]

    def mine(matrix):
        return (v_ref if matrix % 2 == 0 else u_ref).at[matrix // 2]

    def move(matrix, block, number, device, source=None):
        place = piece(matrix, block)
        source = place if source is None else source
        return send(source, place, wss.at[matrix, number], wrs.at[matrix, number], device)

    def far(matrix):
        source = mine(matrix)
        return [
            move(matrix, own, 0, y_far, source),
            move(matrix, own, 1, z_right, source),
            move(matrix, own, 2, z_left, source),
            move(matrix, own, 14, partner, source),
        ]

    def near(matrix):
        block = other + z
        return [move(matrix, block, 3, z_right), move(matrix, block, 4, z_left), move(matrix, block, 7, partner)]

    def onward(matrix):
        return [
            move(matrix, same + zl, 5, z_right),
            move(matrix, other + zr, 6, z_left),
            move(matrix, same + zl, 8, partner),
            move(matrix, same + zr, 9, partner),
            move(matrix, other + zl, 10, partner),
            move(matrix, other + zr, 11, partner),
        ]

    def last(matrix):
        return [move(matrix, same + zo, 12, partner), move(matrix, other + zo, 13, partner)]

    def arrived(matrix, numbers):
        for number in numbers:
            move(matrix, own, number, partner).wait_recv()

    def start(copies):
        for copy in copies:
            copy.start()

    def weights_0(matrix):
        start(far(matrix))
        first = pl.multiple_of(own * block_width + core * share, share)
        w_full[matrix, pl.ds(first, share), :] = mine(matrix)[...]

    def weights_1(matrix):
        arrived(matrix, (0,))
        start(near(matrix))

    def weights_2(matrix):
        arrived(matrix, (1, 2, 3, 4))
        start(onward(matrix))

    def weights_3(matrix):
        arrived(matrix, (5, 6))
        start(last(matrix))

    def weights_4(matrix):
        arrived(matrix, (7, 8, 9, 10, 11, 12, 13, 14))

    weight_stages = (weights_0, weights_1, weights_2, weights_3, weights_4)

    def weights(stage, matrix):
        with jax.named_scope(f"w{stage}_{matrix}"):
            weight_stages[stage](matrix)

    upper, lower = pl.ds(0, half), pl.ds(half, half)

    def first_hop(t):
        return [
            send(part.at[t, xo, upper], rs1.at[t, 0], ss.at[t, 0], rs.at[t, 0], right),
            send(part.at[t, xo, lower], rs1.at[t, 2], ss.at[t, 2], rs.at[t, 2], left),
            send(part.at[t, xr, lower], rs1.at[t, 1], ss.at[t, 1], rs.at[t, 1], right),
            send(part.at[t, xl, upper], rs1.at[t, 3], ss.at[t, 3], rs.at[t, 3], left),
        ]

    def second_hop(t):
        return [
            send(s2.at[t, 0], rs2.at[t, 0], ss.at[t, 4], rs.at[t, 4], right),
            send(s2.at[t, 1], rs2.at[t, 1], ss.at[t, 5], rs.at[t, 5], left),
        ]

    def exchange(t):
        return [send(ysend.at[t], yrecv.at[t], ss.at[t, 6], rs.at[t, 6], across)]

    def share_1(t):
        return [
            send(rank.at[t, x], rank.at[t, x], ss.at[t, 7], rs.at[t, 7], right),
            send(rank.at[t, x], rank.at[t, x], ss.at[t, 8], rs.at[t, 8], left),
        ]

    def share_2(t):
        return [
            send(rank.at[t, xl, upper], rank.at[t, xl, upper], ss.at[t, 9], rs.at[t, 9], right),
            send(rank.at[t, xr, lower], rank.at[t, xr, lower], ss.at[t, 10], rs.at[t, 10], left),
        ]

    def stage_0(t):
        layer, chunk = t // CHUNKS, lax.rem(t, CHUNKS)
        for q in range(4):
            part[t, q] = lax.dot_general(
                carried[chunk],
                w_full[2 * layer, q * quarter : (q + 1) * quarter, :],
                (((1,), (1,)), ((), ())),
                preferred_element_type=F32,
            ).astype(BF16)
        start(first_hop(t))

    def stage_1(t):
        hop = first_hop(t)
        hop[0].wait_recv()
        s2[t, 0] = (part[t, xr, upper].astype(F32) + rs1[t, 0].astype(F32)).astype(BF16)
        hop[1].wait_recv()
        s2[t, 1] = (part[t, xl, lower].astype(F32) + rs1[t, 2].astype(F32)).astype(BF16)
        start(second_hop(t))

    def stage_2(t):
        hop = first_hop(t)
        hop[2].wait_recv()
        hop[3].wait_recv()
        for copy in second_hop(t):
            copy.wait_recv()
        ysend[t, upper] = (
            part[t, x, upper].astype(F32) + rs2[t, 0].astype(F32) + rs1[t, 3].astype(F32)
        ).astype(BF16)
        ysend[t, lower] = (
            part[t, x, lower].astype(F32) + rs2[t, 1].astype(F32) + rs1[t, 1].astype(F32)
        ).astype(BF16)
        start(exchange(t))

    def stage_3(t):
        exchange(t)[0].wait_recv()
        rank[t, x] = (ysend[t].astype(F32) + yrecv[t].astype(F32)).astype(BF16)
        start(share_1(t))

    def stage_4(t):
        for copy in share_1(t):
            copy.wait_recv()
        start(share_2(t))

    def stage_5(t):
        layer, chunk = t // CHUNKS, lax.rem(t, CHUNKS)
        for copy in share_2(t):
            copy.wait_recv()
        where = pl.ds(pl.multiple_of(chunk * rows, rows), rows)
        for j in range(4):
            columns = slice(j * depth // 4, (j + 1) * depth // 4)
            total = b_ref[pl.ds(layer, 1), columns]
            for q in range(4):
                total = total + jnp.dot(
                    rank[t, q],
                    w_full[2 * layer + 1, q * quarter : (q + 1) * quarter, columns],
                    preferred_element_type=F32,
                )
            carried[chunk, :, columns] = (
                f_ref[where, columns].astype(F32) * total + carried[chunk, :, columns].astype(F32)
            ).astype(BF16)

        @pl.when(layer == layers - 1)
        def _():
            out_ref[where, :] = carried[chunk]

    weights(0, 0)

    @pl.loop(0, CHUNKS)
    def _(chunk):
        carried[chunk] = f_ref[pl.ds(pl.multiple_of(chunk * rows, rows), rows), :]

    weights(1, 0)
    weights(2, 0)
    weights(3, 0)
    weights(0, 1)
    weights(1, 1)
    weights(4, 0)

    plan = {}
    for stage in range(2, 5):
        plan.setdefault(stage - 2, []).append((stage, 1))
    for matrix, begin in ((2, 2), (3, 6), (4, 9), (5, 13)):
        for stage in range(5):
            plan.setdefault(begin + stage, []).append((stage, matrix))

    @pl.loop(0, tasks + LAG[5])
    def _(i):
        for when, steps in sorted(plan.items()):
            @pl.when(i == when)
            def _(steps=steps):
                for stage, matrix in steps:
                    weights(stage, matrix)

        for number, stage in ((4, stage_4), (3, stage_3), (2, stage_2), (1, stage_1), (5, stage_5), (0, stage_0)):
            t = i - LAG[number]

            @pl.when(jnp.logical_and(t >= 0, t < tasks))
            def _(number=number, stage=stage, t=t):
                with jax.named_scope(f"s{number}"):
                    stage(t)

    @pl.loop(0, tasks)
    def _(t):
        for copies in (first_hop, second_hop, exchange, share_1, share_2):
            for copy in copies(t):
                copy.wait_send()

    for matrix in range(2 * layers):
        for copies in (far, near, onward, last):
            for copy in copies(matrix):
                copy.wait_send()


def local(features, v_weight, u_weight, cross_bias):
    layers, depth, share = v_weight.shape
    rank = share * lax.axis_size("dp")
    rows = features.shape[0] // CHUNKS
    half = rows // 2
    quarter = rank // 4
    tasks = layers * CHUNKS
    dma = pltpu.SemaphoreType.DMA
    vmem = pl.BlockSpec(memory_space=pltpu.VMEM)
    return pl.pallas_call(
        kernel,
        out_shape=jax.ShapeDtypeStruct(features.shape, BF16),
        in_specs=[vmem] * 4,
        out_specs=vmem,
        scratch_shapes=[
            pltpu.VMEM((2 * layers, rank, depth), BF16),
            pltpu.VMEM((CHUNKS, rows, depth), BF16),
            pltpu.VMEM((tasks, 4, rows, quarter), BF16),
            pltpu.VMEM((tasks, 4, rows, quarter), BF16),
            pltpu.VMEM((tasks, 4, half, quarter), BF16),
            pltpu.VMEM((tasks, 2, half, quarter), BF16),
            pltpu.VMEM((tasks, 2, half, quarter), BF16),
            pltpu.VMEM((tasks, rows, quarter), BF16),
            pltpu.VMEM((tasks, rows, quarter), BF16),
            dma((tasks, 11)),
            dma((tasks, 11)),
            dma((2 * layers, 15)),
            dma((2 * layers, 15)),
        ],
        compiler_params=pltpu.CompilerParams(
            collective_id=0, has_side_effects=True, vmem_limit_bytes=67043328
        ),
    )(features, jnp.swapaxes(v_weight, 1, 2), u_weight, cross_bias)


def solution(mesh):
    return jax.shard_map(
        local,
        mesh=mesh,
        in_specs=(P("dp", "mp"), P(None, "mp", "dp"), P(None, "dp", "mp"), P(None, "mp")),
        out_specs=P("dp", "mp"),
        check_vma=False,
    )
```

```python
import jax
import jax.numpy as jnp
from jax import lax
from jax.experimental import pallas as pl
from jax.experimental.pallas import tpu as pltpu
from jax.sharding import PartitionSpec as P

MESH = pl.DeviceIdType.MESH
BF16 = jnp.bfloat16
F32 = jnp.float32

CHUNKS = 8
LAG = (0, 1, 2, 3, 4, 5)
ORDER = (4, 3, 2, 1, 5, 0)


def kernel(
    f_hbm, v_hbm, u_hbm, b_ref, out_hbm,
    features, w_full, carried, part, rank, rs1, s2, rs2, ysend, yrecv,
    ss, rs, wss, wrs, in_sem, own_sem, out_sem,
):
    layers = v_hbm.shape[0]
    matrices = 2 * layers
    rows = f_hbm.shape[0] // CHUNKS
    half = rows // 2
    depth = f_hbm.shape[1]
    share = u_hbm.shape[1]
    block_width = 2 * share
    tasks = layers * CHUNKS
    quarter = w_full.shape[1] // 4

    dp, mp = lax.axis_index("dp"), lax.axis_index("mp")
    y_hi, z, core = dp // 8, lax.rem(dp // 2, 4), lax.rem(dp, 2)
    y_lo, x = mp // 4, lax.rem(mp, 4)
    xr, xl, xo = lax.rem(x + 1, 4), lax.rem(x + 3, 4), lax.rem(x + 2, 4)
    zr, zl, zo = lax.rem(z + 1, 4), lax.rem(z + 3, 4), lax.rem(z + 2, 4)

    def at(y_hi=y_hi, z=z, core=core, y_lo=y_lo, x=x):
        return ((y_hi * 4 + z) * 2 + core, y_lo * 4 + x)

    right, left, across = at(x=xr), at(x=xl), at(y_lo=1 - y_lo)
    z_right, z_left, y_far, partner = at(z=zr), at(z=zl), at(y_hi=1 - y_hi), at(core=1 - core)

    barrier = pltpu.get_barrier_semaphore()
    for device in (right, left, across, z_right, z_left, y_far, partner):
        pl.semaphore_signal(barrier, inc=1, device_id=device, device_id_type=MESH)

    def send(src, dst, send_sem, recv_sem, device):
        return pltpu.make_async_remote_copy(
            src_ref=src, dst_ref=dst, send_sem=send_sem, recv_sem=recv_sem,
            device_id=device, device_id_type=MESH,
        )

    def start(copies):
        for copy in copies:
            copy.start()

    own, same, other = y_hi * 4 + z, y_hi * 4, (1 - y_hi) * 4

    def piece(matrix, block):
        first = pl.multiple_of(block * block_width + core * share, share)
        return w_full.at[matrix, pl.ds(first, share), :]

    def move(matrix, block, number, device):
        place = piece(matrix, block)
        return send(place, place, wss, wrs.at[matrix, number], device)

    def arrived(matrix, number, pieces):
        place = w_full.at[matrix, pl.ds(0, pieces * share), :]
        send(place, place, wss, wrs.at[matrix, number], partner).wait_recv()

    def own_piece(matrix):
        source = v_hbm if matrix % 2 == 0 else u_hbm
        return pltpu.make_async_copy(source.at[matrix // 2], piece(matrix, own), own_sem.at[matrix])

    def weights_0(matrix):
        start([move(matrix, own, 0, y_far), move(matrix, own, 1, z_right), move(matrix, own, 1, z_left),
               move(matrix, own, 4, partner)])

    def weights_1(matrix):
        arrived(matrix, 1, 2)
        start([move(matrix, same + zl, 3, z_right), move(matrix, same + zl, 4, partner),
               move(matrix, same + zr, 4, partner)])
        arrived(matrix, 0, 1)
        start([move(matrix, other + z, 2, z_right), move(matrix, other + z, 2, z_left),
               move(matrix, other + z, 4, partner)])

    def weights_2(matrix):
        arrived(matrix, 2, 2)
        start([move(matrix, other + zr, 3, z_left), move(matrix, other + zl, 4, partner),
               move(matrix, other + zr, 4, partner)])

    def weights_3(matrix):
        arrived(matrix, 3, 2)
        start([move(matrix, same + zo, 4, partner), move(matrix, other + zo, 4, partner)])

    def weights_4(matrix):
        arrived(matrix, 4, 8)

    weight_stages = (weights_0, weights_1, weights_2, weights_3, weights_4)
    weight_sends = 4 + 6 + 3 + 2

    upper, lower = pl.ds(0, half), pl.ds(half, half)

    def first_hop(t):
        start([
            send(part.at[t, xo, upper], rs1.at[t, 0], ss.at[0], rs.at[t, 0], right),
            send(part.at[t, xo, lower], rs1.at[t, 2], ss.at[0], rs.at[t, 0], left),
            send(part.at[t, xr, lower], rs1.at[t, 1], ss.at[0], rs.at[t, 1], right),
            send(part.at[t, xl, upper], rs1.at[t, 3], ss.at[0], rs.at[t, 1], left),
        ])

    def second_hop(t):
        start([
            send(s2.at[t, 0], rs2.at[t, 0], ss.at[1], rs.at[t, 1], right),
            send(s2.at[t, 1], rs2.at[t, 1], ss.at[1], rs.at[t, 1], left),
        ])

    def exchange(t):
        start([send(ysend.at[t], yrecv.at[t], ss.at[2], rs.at[t, 2], across)])

    def share_1(t):
        start([
            send(rank.at[t, x], rank.at[t, x], ss.at[3], rs.at[t, 3], right),
            send(rank.at[t, x], rank.at[t, x], ss.at[3], rs.at[t, 3], left),
        ])

    def share_2(t):
        start([
            send(rank.at[t, xl, upper], rank.at[t, xl, upper], ss.at[4], rs.at[t, 4], right),
            send(rank.at[t, xr, lower], rank.at[t, xr, lower], ss.at[4], rs.at[t, 4], left),
        ])

    def await_recv(t, number, size):
        send(size.at[t], size.at[t], ss.at[0], rs.at[t, number], right).wait_recv()

    def chunk_rows(chunk):
        return pl.ds(pl.multiple_of(chunk * rows, rows), rows)

    def result(chunk):
        return pltpu.make_async_copy(carried.at[chunk], out_hbm.at[chunk_rows(chunk), :], out_sem.at[0])

    def stage_0(t):
        layer, chunk = t // CHUNKS, lax.rem(t, CHUNKS)
        for q in range(4):
            part[t, q] = lax.dot_general(
                carried[chunk],
                w_full[2 * layer, q * quarter : (q + 1) * quarter, :],
                (((1,), (1,)), ((), ())),
                preferred_element_type=F32,
            ).astype(BF16)
        first_hop(t)

    def stage_1(t):
        await_recv(t, 0, rs2)
        s2[t, 0] = (part[t, xr, upper].astype(F32) + rs1[t, 0].astype(F32)).astype(BF16)
        s2[t, 1] = (part[t, xl, lower].astype(F32) + rs1[t, 2].astype(F32)).astype(BF16)
        second_hop(t)

    def stage_2(t):
        await_recv(t, 1, rs1)
        ysend[t, upper] = (
            part[t, x, upper].astype(F32) + rs2[t, 0].astype(F32) + rs1[t, 3].astype(F32)
        ).astype(BF16)
        ysend[t, lower] = (
            part[t, x, lower].astype(F32) + rs2[t, 1].astype(F32) + rs1[t, 1].astype(F32)
        ).astype(BF16)
        exchange(t)

    def stage_3(t):
        await_recv(t, 2, yrecv)
        rank[t, x] = (ysend[t].astype(F32) + yrecv[t].astype(F32)).astype(BF16)
        share_1(t)

    def stage_4(t):
        await_recv(t, 3, rs1)
        share_2(t)

    def stage_5(t):
        layer, chunk = t // CHUNKS, lax.rem(t, CHUNKS)
        await_recv(t, 4, rs2)
        for j in range(4):
            columns = slice(j * depth // 4, (j + 1) * depth // 4)
            total = b_ref[pl.ds(layer, 1), columns]
            for q in range(4):
                total = total + jnp.dot(
                    rank[t, q],
                    w_full[2 * layer + 1, q * quarter : (q + 1) * quarter, columns],
                    preferred_element_type=F32,
                )
            carried[chunk, :, columns] = (
                features[chunk_rows(chunk), columns].astype(F32) * total + carried[chunk, :, columns].astype(F32)
            ).astype(BF16)

        @pl.when(layer == layers - 1)
        def _():
            result(chunk).start()

    stages = (stage_0, stage_1, stage_2, stage_3, stage_4, stage_5)

    for matrix in range(matrices):
        own_piece(matrix).start()
    fetches = [pltpu.make_async_copy(f_hbm, features, in_sem.at[0])] + [
        pltpu.make_async_copy(f_hbm.at[pl.ds(chunk * rows, rows), :], carried.at[chunk], in_sem.at[1])
        for chunk in range(CHUNKS)
    ]
    start(fetches)
    with jax.named_scope("barrier"):
        pl.semaphore_wait(barrier, 7)
    with jax.named_scope("fetch"):
        for matrix in range(matrices):
            own_piece(matrix).wait()
    with jax.named_scope("v0"):
        weights_0(0)
        weights_1(0)
        weights_2(0)
    weights_0(1)
    with jax.named_scope("v0b"):
        weights_3(0)
    with jax.named_scope("u0"):
        weights_1(1)
    with jax.named_scope("v0c"):
        weights_4(0)
        for fetch in fetches:
            fetch.wait()

    @pl.loop(0, tasks + LAG[5])
    def _(i):
        for number in ORDER:
            t = i - LAG[number]

            @pl.when(jnp.logical_and(t >= 0, t < tasks))
            def _(number=number, t=t):
                with jax.named_scope(f"s{number}"):
                    stages[number](t)

        for number in range(5):
            turn = i + 6 - number
            matrix = turn // 4

            @pl.when(jnp.logical_and(lax.rem(turn, 4) == 0, jnp.logical_and(matrix >= 1, matrix < matrices)))
            def _(number=number, matrix=matrix):
                with jax.named_scope(f"w{number}"):
                    weight_stages[number](matrix)

    with jax.named_scope("end"):
        for number, size in ((0, rs1), (1, rs2), (2, yrecv), (3, rs1), (4, rs2)):
            send(size, size, ss.at[number], rs.at[0, 0], right).wait_send()
        for matrix in range(matrices):
            place = w_full.at[matrix, pl.ds(0, weight_sends * share), :]
            send(place, place, wss, wrs.at[0, 0], right).wait_send()
        for chunk in range(CHUNKS):
            result(chunk).wait()


def local(features, v_weight, u_weight, cross_bias):
    layers, depth, share = v_weight.shape
    rank = share * lax.axis_size("dp")
    rows = features.shape[0] // CHUNKS
    half = rows // 2
    quarter = rank // 4
    tasks = layers * CHUNKS
    dma = pltpu.SemaphoreType.DMA
    anywhere = pl.BlockSpec(memory_space=pl.ANY)
    return pl.pallas_call(
        kernel,
        out_shape=jax.ShapeDtypeStruct(features.shape, BF16),
        in_specs=[anywhere] * 3 + [pl.BlockSpec(memory_space=pltpu.VMEM)],
        out_specs=anywhere,
        scratch_shapes=[
            pltpu.VMEM(features.shape, BF16),
            pltpu.VMEM((2 * layers, rank, depth), BF16),
            pltpu.VMEM((CHUNKS, rows, depth), BF16),
            pltpu.VMEM((tasks, 4, rows, quarter), BF16),
            pltpu.VMEM((tasks, 4, rows, quarter), BF16),
            pltpu.VMEM((tasks, 4, half, quarter), BF16),
            pltpu.VMEM((tasks, 2, half, quarter), BF16),
            pltpu.VMEM((tasks, 2, half, quarter), BF16),
            pltpu.VMEM((tasks, rows, quarter), BF16),
            pltpu.VMEM((tasks, rows, quarter), BF16),
            dma((5,)),
            dma((tasks, 5)),
            dma,
            dma((2 * layers, 5)),
            dma((2,)),
            dma((2 * layers,)),
            dma((1,)),
        ],
        compiler_params=pltpu.CompilerParams(
            collective_id=0, has_side_effects=True, vmem_limit_bytes=67043328
        ),
    )(features, jnp.swapaxes(v_weight, 1, 2), u_weight, cross_bias)


def solution(mesh):
    return jax.shard_map(
        local,
        mesh=mesh,
        in_specs=(P("dp", "mp"), P(None, "mp", "dp"), P(None, "dp", "mp"), P(None, "mp")),
        out_specs=P("dp", "mp"),
        check_vma=False,
    )
```

```python
import jax
import jax.numpy as jnp
from jax import lax
from jax.experimental import pallas as pl
from jax.experimental.pallas import tpu as pltpu
from jax.sharding import PartitionSpec as P

MESH = pl.DeviceIdType.MESH
BF16 = jnp.bfloat16
F32 = jnp.float32

CHUNKS = 8
LAG = (0, 1, 2, 3, 4, 5, 6)
WLAG = (0, 3, 5, 7, 8)
EARLY = 32
UPPER_A, UPPER_B = 16, 48


def kernel(
    f_hbm, v_hbm, u_hbm, b_ref, out_hbm,
    features, w_full, carried,
    part_b, far_b, mid_b, near_b, sum_b, across_b, rank_b,
    part_a, across_a, sum_a, far_a, mid_a, near_a, rank_a,
    ss, rs, wss, wrs, in_sem, own_sem, out_sem,
):
    layers = v_hbm.shape[0]
    matrices = 2 * layers
    rows = f_hbm.shape[0] // CHUNKS
    late = rows - EARLY
    depth = f_hbm.shape[1]
    share = u_hbm.shape[1]
    block_width = 2 * share
    tasks = layers * CHUNKS
    quarter = w_full.shape[1] // 4

    dp, mp = lax.axis_index("dp"), lax.axis_index("mp")
    y_hi, z, core = dp // 8, lax.rem(dp // 2, 4), lax.rem(dp, 2)
    y_lo, x = mp // 4, lax.rem(mp, 4)
    xr, xl, xo = lax.rem(x + 1, 4), lax.rem(x + 3, 4), lax.rem(x + 2, 4)
    zr, zl, zo = lax.rem(z + 1, 4), lax.rem(z + 3, 4), lax.rem(z + 2, 4)

    def at(y_hi=y_hi, z=z, core=core, y_lo=y_lo, x=x):
        return ((y_hi * 4 + z) * 2 + core, y_lo * 4 + x)

    right, left, across = at(x=xr), at(x=xl), at(y_lo=1 - y_lo)
    z_right, z_left, y_far, partner = at(z=zr), at(z=zl), at(y_hi=1 - y_hi), at(core=1 - core)

    barrier = pltpu.get_barrier_semaphore()
    for device in (right, left, across, z_right, z_left, y_far, partner):
        pl.semaphore_signal(barrier, inc=1, device_id=device, device_id_type=MESH)

    def send(src, dst, send_sem, recv_sem, device):
        return pltpu.make_async_remote_copy(
            src_ref=src, dst_ref=dst, send_sem=send_sem, recv_sem=recv_sem,
            device_id=device, device_id_type=MESH,
        )

    def start(copies):
        for copy in copies:
            copy.start()

    own, same, other = y_hi * 4 + z, y_hi * 4, (1 - y_hi) * 4

    def piece(matrix, block):
        first = pl.multiple_of(block * block_width + core * share, share)
        return w_full.at[matrix, pl.ds(first, share), :]

    def move(matrix, block, number, device):
        place = piece(matrix, block)
        return send(place, place, wss, wrs.at[matrix, number], device)

    def arrived(matrix, number, pieces):
        place = w_full.at[matrix, pl.ds(0, pieces * share), :]
        send(place, place, wss, wrs.at[matrix, number], partner).wait_recv()

    def own_piece(matrix):
        source = v_hbm if matrix % 2 == 0 else u_hbm
        return pltpu.make_async_copy(source.at[matrix // 2], piece(matrix, own), own_sem.at[matrix])

    def weights_0(matrix):
        start([move(matrix, own, 0, y_far), move(matrix, own, 1, z_right), move(matrix, own, 1, z_left),
               move(matrix, own, 4, partner)])

    def weights_1(matrix):
        arrived(matrix, 1, 2)
        start([move(matrix, same + zl, 3, z_right), move(matrix, same + zl, 4, partner),
               move(matrix, same + zr, 4, partner)])
        arrived(matrix, 0, 1)
        start([move(matrix, other + z, 2, z_right), move(matrix, other + z, 2, z_left),
               move(matrix, other + z, 4, partner)])

    def weights_2(matrix):
        arrived(matrix, 2, 2)
        start([move(matrix, other + zr, 3, z_left), move(matrix, other + zl, 4, partner),
               move(matrix, other + zr, 4, partner)])

    def weights_3(matrix):
        arrived(matrix, 3, 2)
        start([move(matrix, same + zo, 4, partner), move(matrix, other + zo, 4, partner)])

    def weights_4(matrix):
        arrived(matrix, 4, 8)

    weight_stages = (weights_0, weights_1, weights_2, weights_3, weights_4)
    weight_sends = 4 + 6 + 3 + 2

    def to_right_and_left(t, rows, upper, part, far, mid, near, rank, first):
        upper, lower = pl.ds(0, upper), pl.ds(upper, rows - upper)

        def hop_1():
            start([
                send(part(xo).at[upper], far.at[t, upper], ss.at[first], rs.at[t, first], right),
                send(part(xo).at[lower], far.at[t, lower], ss.at[first], rs.at[t, first], left),
                send(part(xr).at[lower], near.at[t, 0, lower], ss.at[first], rs.at[t, first + 1], right),
                send(part(xl).at[upper], near.at[t, 0, upper], ss.at[first], rs.at[t, first + 1], left),
            ])

        def hop_2():
            await_recv(t, first, far)
            mid[t, upper] = (part(xr)[upper].astype(F32) + far[t, upper].astype(F32)).astype(BF16)
            mid[t, lower] = (part(xl)[lower].astype(F32) + far[t, lower].astype(F32)).astype(BF16)
            start([
                send(mid.at[t, upper], near.at[t, 1, upper], ss.at[first + 1], rs.at[t, first + 1], right),
                send(mid.at[t, lower], near.at[t, 1, lower], ss.at[first + 1], rs.at[t, first + 1], left),
            ])

        def total():
            await_recv(t, first + 1, near)
            return (
                part(x)[...].astype(F32) + near[t, 0].astype(F32) + near[t, 1].astype(F32)
            ).astype(BF16)

        def share_1():
            start([
                send(rank(x), rank(x), ss.at[first + 2], rs.at[t, first + 2], right),
                send(rank(x), rank(x), ss.at[first + 2], rs.at[t, first + 2], left),
            ])

        def share_2():
            await_recv(t, first + 2, near)
            start([
                send(rank(xl).at[lower], rank(xl).at[lower], ss.at[first + 3], rs.at[t, first + 3], right),
                send(rank(xr).at[upper], rank(xr).at[upper], ss.at[first + 3], rs.at[t, first + 3], left),
            ])

        return hop_1, hop_2, total, share_1, share_2

    def ways(t):
        late_ways = to_right_and_left(
            t, late, UPPER_B, lambda q: part_b.at[t, q], far_b, mid_b, near_b, lambda q: rank_b.at[t, q], 0
        )
        early_ways = to_right_and_left(
            t, EARLY, UPPER_A, lambda q: sum_a.at[t, q], far_a, mid_a, near_a, lambda q: rank_a.at[t, y_lo, q], 4
        )
        return late_ways, early_ways

    def over_y(t, src, dst, number):
        send(src, dst, ss.at[number], rs.at[t, number], across).start()

    def await_recv(t, number, size):
        send(size.at[t], size.at[t], ss.at[0], rs.at[t, number], right).wait_recv()

    def chunk_rows(chunk):
        return pl.ds(pl.multiple_of(chunk * rows, rows), rows)

    def result(chunk):
        return pltpu.make_async_copy(carried.at[chunk], out_hbm.at[chunk_rows(chunk), :], out_sem.at[0])

    def stage_0(t):
        layer, chunk = t // CHUNKS, lax.rem(t, CHUNKS)
        for q in range(4):
            piece_q = lax.dot_general(
                carried[chunk],
                w_full[2 * layer, q * quarter : (q + 1) * quarter, :],
                (((1,), (1,)), ((), ())),
                preferred_element_type=F32,
            ).astype(BF16)
            part_b[t, q] = piece_q[:late]
            part_a[t, 0, q] = piece_q[late:, : quarter // 2]
            part_a[t, 1, q] = piece_q[late:, quarter // 2 :]
        over_y(t, part_a.at[t, 1 - y_lo], across_a.at[t], 9)
        ways(t)[0][0]()

    def stage_1(t):
        late_ways, early_ways = ways(t)
        await_recv(t, 9, across_a)
        sum_a[t] = (part_a[t, y_lo].astype(F32) + across_a[t].astype(F32)).astype(BF16)
        early_ways[0]()
        late_ways[1]()

    def stage_2(t):
        late_ways, early_ways = ways(t)
        early_ways[1]()
        sum_b[t] = late_ways[2]()
        over_y(t, sum_b.at[t], across_b.at[t], 8)

    def stage_3(t):
        late_ways, early_ways = ways(t)
        rank_a[t, y_lo, x] = early_ways[2]()
        early_ways[3]()
        await_recv(t, 8, across_b)
        rank_b[t, x] = (sum_b[t].astype(F32) + across_b[t].astype(F32)).astype(BF16)
        late_ways[3]()

    def stage_4(t):
        late_ways, early_ways = ways(t)
        early_ways[4]()
        late_ways[4]()

    def stage_5(t):
        await_recv(t, 7, far_a)
        over_y(t, rank_a.at[t, y_lo], rank_a.at[t, y_lo], 10)

    def stage_6(t):
        layer, chunk = t // CHUNKS, lax.rem(t, CHUNKS)
        await_recv(t, 3, far_b)
        await_recv(t, 10, across_a)
        lhs = [
            jnp.concatenate(
                [rank_b[t, q], jnp.concatenate([rank_a[t, 0, q], rank_a[t, 1, q]], axis=1)], axis=0
            )
            for q in range(4)
        ]
        for j in range(4):
            columns = slice(j * depth // 4, (j + 1) * depth // 4)
            total = b_ref[pl.ds(layer, 1), columns]
            for q in range(4):
                total = total + jnp.dot(
                    lhs[q],
                    w_full[2 * layer + 1, q * quarter : (q + 1) * quarter, columns],
                    preferred_element_type=F32,
                )
            carried[chunk, :, columns] = (
                features[chunk_rows(chunk), columns].astype(F32) * total + carried[chunk, :, columns].astype(F32)
            ).astype(BF16)

        @pl.when(layer == layers - 1)
        def _():
            result(chunk).start()

    stages = (stage_0, stage_1, stage_2, stage_3, stage_4, stage_5, stage_6)

    for matrix in range(matrices):
        own_piece(matrix).start()
    fetches = [pltpu.make_async_copy(f_hbm, features, in_sem.at[0])] + [
        pltpu.make_async_copy(f_hbm.at[pl.ds(chunk * rows, rows), :], carried.at[chunk], in_sem.at[1])
        for chunk in range(CHUNKS)
    ]
    start(fetches)
    with jax.named_scope("barrier"):
        pl.semaphore_wait(barrier, 7)
    with jax.named_scope("fetch"):
        for matrix in range(matrices):
            own_piece(matrix).wait()
    with jax.named_scope("v0"):
        weights_0(0)
        weights_1(0)
        weights_2(0)
    weights_0(1)
    with jax.named_scope("v0b"):
        weights_3(0)
    with jax.named_scope("v0c"):
        weights_4(0)
        for fetch in fetches:
            fetch.wait()

    def weights_at(i, number):
        turn = i - WLAG[number]
        first = turn == -WLAG[1]
        matrix = jnp.where(first, 1, turn // 4 + 2)
        regular = jnp.logical_and(jnp.logical_and(turn >= 0, lax.rem(turn, 4) == 0), matrix < matrices)

        @pl.when(jnp.logical_or(first, regular))
        def _():
            with jax.named_scope(f"w{number}"):
                weight_stages[number](matrix)

    @pl.loop(0, tasks + LAG[6])
    def _(i):
        weights_at(i, 4)
        for number in range(7):
            t = i - LAG[number]

            @pl.when(jnp.logical_and(t >= 0, t < tasks))
            def _(number=number, t=t):
                with jax.named_scope(f"s{number}"):
                    stages[number](t)

        for number in range(4):
            weights_at(i, number)

    with jax.named_scope("end"):
        sent = (
            near_b, far_b, near_b, far_b, near_a, far_a, near_a, far_a, across_b, across_a, across_a
        )
        for number, size in enumerate(sent):
            send(size, size, ss.at[number], rs.at[0, 0], right).wait_send()
        for matrix in range(matrices):
            place = w_full.at[matrix, pl.ds(0, weight_sends * share), :]
            send(place, place, wss, wrs.at[0, 0], right).wait_send()
        for chunk in range(CHUNKS):
            result(chunk).wait()


def local(features, v_weight, u_weight, cross_bias):
    layers, depth, share = v_weight.shape
    rank = share * lax.axis_size("dp")
    rows = features.shape[0] // CHUNKS
    late = rows - EARLY
    quarter = rank // 4
    tasks = layers * CHUNKS
    dma = pltpu.SemaphoreType.DMA
    anywhere = pl.BlockSpec(memory_space=pl.ANY)
    return pl.pallas_call(
        kernel,
        out_shape=jax.ShapeDtypeStruct(features.shape, BF16),
        in_specs=[anywhere] * 3 + [pl.BlockSpec(memory_space=pltpu.VMEM)],
        out_specs=anywhere,
        scratch_shapes=[
            pltpu.VMEM(features.shape, BF16),
            pltpu.VMEM((2 * layers, rank, depth), BF16),
            pltpu.VMEM((CHUNKS, rows, depth), BF16),
            pltpu.VMEM((tasks, 4, late, quarter), BF16),
            pltpu.VMEM((tasks, late, quarter), BF16),
            pltpu.VMEM((tasks, late, quarter), BF16),
            pltpu.VMEM((tasks, 2, late, quarter), BF16),
            pltpu.VMEM((tasks, late, quarter), BF16),
            pltpu.VMEM((tasks, late, quarter), BF16),
            pltpu.VMEM((tasks, 4, late, quarter), BF16),
            pltpu.VMEM((tasks, 2, 4, EARLY, quarter // 2), BF16),
            pltpu.VMEM((tasks, 4, EARLY, quarter // 2), BF16),
            pltpu.VMEM((tasks, 4, EARLY, quarter // 2), BF16),
            pltpu.VMEM((tasks, EARLY, quarter // 2), BF16),
            pltpu.VMEM((tasks, EARLY, quarter // 2), BF16),
            pltpu.VMEM((tasks, 2, EARLY, quarter // 2), BF16),
            pltpu.VMEM((tasks, 2, 4, EARLY, quarter // 2), BF16),
            dma((11,)),
            dma((tasks, 11)),
            dma,
            dma((2 * layers, 5)),
            dma((2,)),
            dma((2 * layers,)),
            dma((1,)),
        ],
        compiler_params=pltpu.CompilerParams(
            collective_id=0, has_side_effects=True, vmem_limit_bytes=67043328
        ),
    )(features, jnp.swapaxes(v_weight, 1, 2), u_weight, cross_bias)


def solution(mesh):
    return jax.shard_map(
        local,
        mesh=mesh,
        in_specs=(P("dp", "mp"), P(None, "mp", "dp"), P(None, "dp", "mp"), P(None, "mp")),
        out_specs=P("dp", "mp"),
        check_vma=False,
    )
```

```python
import jax
import jax.numpy as jnp
from jax import lax
from jax.experimental import pallas as pl
from jax.experimental.pallas import tpu as pltpu
from jax.sharding import PartitionSpec as P

MESH = pl.DeviceIdType.MESH
BF16 = jnp.bfloat16
F32 = jnp.float32

CHUNKS = 8
LAG = (0, 1, 2, 3, 4, 5, 7)
WLAG = (0, 2, 4, 6, 8)
EARLY = 48
UPPER_A, UPPER_B = 32, 48
SLOTS = 8
PARTS = 4


def kernel(
    f_hbm, v_hbm, u_hbm, b_hbm, out_ref,
    features, w_full, carried, bias,
    part_b, far_b, mid_b, near_b, sum_b, across_b, rank_b,
    part_a, across_a, sum_a, far_a, mid_a, near_a, rank_a,
    ss, rs, wss, wrs, v0s, in_sem, own_sem,
):
    layers = v_hbm.shape[0]
    matrices = 2 * layers
    rows = f_hbm.shape[0] // CHUNKS
    late = rows - EARLY
    depth = f_hbm.shape[1]
    share = u_hbm.shape[1]
    block_width = 2 * share
    tasks = layers * CHUNKS
    quarter = w_full.shape[1] // 4

    dp, mp = lax.axis_index("dp"), lax.axis_index("mp")
    y_hi, z, core = dp // 8, lax.rem(dp // 2, 4), lax.rem(dp, 2)
    y_lo, x = mp // 4, lax.rem(mp, 4)
    xr, xl, xo = lax.rem(x + 1, 4), lax.rem(x + 3, 4), lax.rem(x + 2, 4)
    zr, zl, zo = lax.rem(z + 1, 4), lax.rem(z + 3, 4), lax.rem(z + 2, 4)

    def at(y_hi=y_hi, z=z, core=core, y_lo=y_lo, x=x):
        return ((y_hi * 4 + z) * 2 + core, y_lo * 4 + x)

    right, left, across = at(x=xr), at(x=xl), at(y_lo=1 - y_lo)
    z_right, z_left, y_far, partner = at(z=zr), at(z=zl), at(y_hi=1 - y_hi), at(core=1 - core)

    barrier = pltpu.get_barrier_semaphore()
    for device in (right, left, across, z_right, z_left, y_far, partner):
        pl.semaphore_signal(barrier, inc=1, device_id=device, device_id_type=MESH)

    def send(src, dst, send_sem, recv_sem, device):
        return pltpu.make_async_remote_copy(
            src_ref=src, dst_ref=dst, send_sem=send_sem, recv_sem=recv_sem,
            device_id=device, device_id_type=MESH,
        )

    def start(copies):
        for copy in copies:
            copy.start()

    own, same, other = y_hi * 4 + z, y_hi * 4, (1 - y_hi) * 4

    def piece(matrix, block):
        first = pl.multiple_of(block * block_width + core * share, share)
        return w_full.at[matrix, pl.ds(first, share), :]

    def move(matrix, block, number, device):
        place = piece(matrix, block)
        return send(place, place, wss, wrs.at[matrix, number], device)

    def arrived(matrix, number, pieces):
        place = w_full.at[matrix, pl.ds(0, pieces * share), :]
        send(place, place, wss, wrs.at[matrix, number], partner).wait_recv()

    def own_piece(matrix):
        source = v_hbm if matrix % 2 == 0 else u_hbm
        return pltpu.make_async_copy(source.at[matrix // 2], piece(matrix, own), own_sem.at[matrix])

    def weights_0(matrix):
        start([move(matrix, own, 1, z_right), move(matrix, own, 1, z_left), move(matrix, own, 4, partner)])

    def weights_1(matrix):
        arrived(matrix, 1, 2)
        start([move(matrix, same + zl, 3, z_right), move(matrix, same + zl, 4, partner),
               move(matrix, same + zr, 4, partner)])
        arrived(matrix, 0, 1)
        start([move(matrix, other + z, 2, z_right), move(matrix, other + z, 2, z_left),
               move(matrix, other + z, 4, partner)])

    def weights_2(matrix):
        arrived(matrix, 2, 2)
        start([move(matrix, other + zr, 3, z_left), move(matrix, other + zl, 4, partner),
               move(matrix, other + zr, 4, partner)])

    def weights_3(matrix):
        arrived(matrix, 3, 2)
        start([move(matrix, same + zo, 4, partner), move(matrix, other + zo, 4, partner)])

    def weights_4(matrix):
        arrived(matrix, 4, 8)

    weight_stages = (weights_0, weights_1, weights_2, weights_3, weights_4)
    weight_sends = 4 + 6 + 3 + 2

    def down_0():
        step = share // PARTS

        def sub(block, s, sem, device):
            first = pl.multiple_of(block * block_width + core * share + s * step, step)
            place = w_full.at[0, pl.ds(first, step), :]
            return send(place, place, wss, sem, device)

        def landed(kind, s):
            sub(own, s, v0s.at[kind, s], partner).wait_recv()

        for s in range(PARTS):
            start([sub(own, s, v0s.at[0, s], z_right), sub(own, s, wrs.at[0, 0], z_left), sub(own, s, v0s.at[1, s], y_far)])
        move(0, own, 4, partner).start()
        for matrix in range(1, matrices):
            move(matrix, own, 0, y_far).start()
        for s in range(PARTS):
            landed(0, s)
            sub(same + zl, s, wrs.at[0, 2], z_right).start()
            landed(1, s)
            start([sub(other + z, s, wrs.at[0, 1], z_right), sub(other + z, s, v0s.at[2, s], z_left)])
        start([move(0, same + zl, 4, partner), move(0, other + z, 4, partner)])
        arrived(0, 0, 1)
        move(0, same + zr, 4, partner).start()
        for s in range(PARTS):
            landed(2, s)
            sub(other + zr, s, wrs.at[0, 3], z_left).start()
        move(0, other + zr, 4, partner).start()
        arrived(0, 1, 1)
        move(0, other + zl, 4, partner).start()
        weights_0(1)
        arrived(0, 2, 1)
        move(0, same + zo, 4, partner).start()
        arrived(0, 3, 1)
        move(0, other + zo, 4, partner).start()
        arrived(0, 4, 8)

    def to_right_and_left(t, rows, upper, part, far, mid, near, rank, first):
        upper, lower = pl.ds(0, upper), pl.ds(upper, rows - upper)

        def hop_1():
            start([
                send(part(xo).at[upper], far.at[t, upper], ss.at[first], rs.at[lax.rem(t, SLOTS), first], right),
                send(part(xo).at[lower], far.at[t, lower], ss.at[first], rs.at[lax.rem(t, SLOTS), first], left),
                send(part(xr).at[lower], near.at[t, 0, lower], ss.at[first], rs.at[lax.rem(t, SLOTS), first + 1], right),
                send(part(xl).at[upper], near.at[t, 0, upper], ss.at[first], rs.at[lax.rem(t, SLOTS), first + 1], left),
            ])

        def hop_2():
            await_recv(t, first, far)
            mid[t, upper] = (part(xr)[upper].astype(F32) + far[t, upper].astype(F32)).astype(BF16)
            mid[t, lower] = (part(xl)[lower].astype(F32) + far[t, lower].astype(F32)).astype(BF16)
            start([
                send(mid.at[t, upper], near.at[t, 1, upper], ss.at[first + 1], rs.at[lax.rem(t, SLOTS), first + 1], right),
                send(mid.at[t, lower], near.at[t, 1, lower], ss.at[first + 1], rs.at[lax.rem(t, SLOTS), first + 1], left),
            ])

        def total():
            await_recv(t, first + 1, near)
            return (
                part(x)[...].astype(F32) + near[t, 0].astype(F32) + near[t, 1].astype(F32)
            ).astype(BF16)

        def share_1():
            start([
                send(rank(x), rank(x), ss.at[first + 2], rs.at[lax.rem(t, SLOTS), first + 2], right),
                send(rank(x), rank(x), ss.at[first + 2], rs.at[lax.rem(t, SLOTS), first + 2], left),
            ])

        def share_2():
            await_recv(t, first + 2, near)
            start([
                send(rank(xl).at[lower], rank(xl).at[lower], ss.at[first + 3], rs.at[lax.rem(t, SLOTS), first + 3], right),
                send(rank(xr).at[upper], rank(xr).at[upper], ss.at[first + 3], rs.at[lax.rem(t, SLOTS), first + 3], left),
            ])

        return hop_1, hop_2, total, share_1, share_2

    def ways(t):
        late_ways = to_right_and_left(
            t, late, UPPER_B, lambda q: part_b.at[t, q], far_b, mid_b, near_b, lambda q: rank_b.at[t, q], 0
        )
        early_ways = to_right_and_left(
            t, EARLY, UPPER_A, lambda q: sum_a.at[t, q], far_a, mid_a, near_a, lambda q: rank_a.at[t, y_lo, q], 4
        )
        return late_ways, early_ways

    def over_y(t, src, dst, number):
        send(src, dst, ss.at[number], rs.at[lax.rem(t, SLOTS), number], across).start()

    def await_recv(t, number, size):
        send(size.at[t], size.at[t], ss.at[0], rs.at[lax.rem(t, SLOTS), number], right).wait_recv()

    def chunk_rows(chunk):
        return pl.ds(pl.multiple_of(chunk * rows, rows), rows)

    def stage_0(t):
        layer, chunk = t // CHUNKS, lax.rem(t, CHUNKS)
        for q in range(4):
            piece_q = lax.dot_general(
                carried[chunk],
                w_full[2 * layer, q * quarter : (q + 1) * quarter, :],
                (((1,), (1,)), ((), ())),
                preferred_element_type=F32,
            ).astype(BF16)
            part_b[t, q] = piece_q[:late]
            part_a[t, 0, q] = piece_q[late:, : quarter // 2]
            part_a[t, 1, q] = piece_q[late:, quarter // 2 :]
        over_y(t, part_a.at[t, 1 - y_lo], across_a.at[t], 9)
        ways(t)[0][0]()

    def stage_1(t):
        late_ways, early_ways = ways(t)
        await_recv(t, 9, across_a)
        sum_a[t] = (part_a[t, y_lo].astype(F32) + across_a[t].astype(F32)).astype(BF16)
        early_ways[0]()
        late_ways[1]()

    def stage_2(t):
        late_ways, early_ways = ways(t)
        early_ways[1]()
        sum_b[t] = late_ways[2]()
        over_y(t, sum_b.at[t], across_b.at[t], 8)

    def stage_3(t):
        late_ways, early_ways = ways(t)
        rank_a[t, y_lo, x] = early_ways[2]()
        early_ways[3]()
        await_recv(t, 8, across_b)
        rank_b[t, x] = (sum_b[t].astype(F32) + across_b[t].astype(F32)).astype(BF16)
        late_ways[3]()

    def stage_4(t):
        late_ways, early_ways = ways(t)
        early_ways[4]()
        late_ways[4]()

    def stage_5(t):
        await_recv(t, 7, far_a)
        over_y(t, rank_a.at[t, y_lo], rank_a.at[t, y_lo], 10)

    def stage_6(t):
        layer, chunk = t // CHUNKS, lax.rem(t, CHUNKS)
        await_recv(t, 3, far_b)
        await_recv(t, 10, across_a)
        lhs = [
            jnp.concatenate(
                [rank_b[t, q], jnp.concatenate([rank_a[t, 0, q], rank_a[t, 1, q]], axis=1)], axis=0
            )
            for q in range(4)
        ]
        for j in range(4):
            columns = slice(j * depth // 4, (j + 1) * depth // 4)
            total = bias[pl.ds(layer, 1), columns]
            for q in range(4):
                total = total + jnp.dot(
                    lhs[q],
                    w_full[2 * layer + 1, q * quarter : (q + 1) * quarter, columns],
                    preferred_element_type=F32,
                )
            new = (
                features[chunk_rows(chunk), columns].astype(F32) * total + carried[chunk, :, columns].astype(F32)
            ).astype(BF16)
            carried[chunk, :, columns] = new

            @pl.when(layer == layers - 1)
            def _(columns=columns, new=new):
                out_ref[chunk_rows(chunk), columns] = new

    stages = (stage_0, stage_1, stage_2, stage_3, stage_4, stage_5, stage_6)

    for matrix in range(matrices):
        own_piece(matrix).start()
    fetches = [pltpu.make_async_copy(f_hbm, features, in_sem.at[0]), pltpu.make_async_copy(b_hbm, bias, in_sem.at[2])] + [
        pltpu.make_async_copy(f_hbm.at[pl.ds(chunk * rows, rows), :], carried.at[chunk], in_sem.at[1])
        for chunk in range(CHUNKS)
    ]
    start(fetches)
    with jax.named_scope("barrier"):
        pl.semaphore_wait(barrier, 7)
    with jax.named_scope("fetch"):
        for matrix in range(matrices):
            own_piece(matrix).wait()
    with jax.named_scope("v0"):
        down_0()
    with jax.named_scope("v0c"):
        for fetch in fetches:
            fetch.wait()

    def weights_at(i, number):
        turn = i - WLAG[number]
        first = turn == -WLAG[1]
        matrix = jnp.where(first, 1, turn // 4 + 2)
        regular = jnp.logical_and(jnp.logical_and(turn >= 0, lax.rem(turn, 4) == 0), matrix < matrices)

        @pl.when(jnp.logical_or(first, regular))
        def _():
            with jax.named_scope(f"w{number}"):
                weight_stages[number](matrix)

    @pl.loop(0, tasks + LAG[6])
    def _(i):
        weights_at(i, 4)
        for number in range(7):
            t = i - LAG[number]

            @pl.when(jnp.logical_and(t >= 0, t < tasks))
            def _(number=number, t=t):
                with jax.named_scope(f"s{number}"):
                    stages[number](t)

        for number in range(4):
            weights_at(i, number)

    with jax.named_scope("end"):
        sent = (
            near_b, far_b, near_b, far_b, near_a, far_a, near_a, far_a, across_b, across_a, across_a
        )
        for number, size in enumerate(sent):
            send(size, size, ss.at[number], rs.at[0, 0], right).wait_send()
        for matrix in range(matrices):
            place = w_full.at[matrix, pl.ds(0, weight_sends * share), :]
            send(place, place, wss, wrs.at[0, 0], right).wait_send()


def local(features, v_weight, u_weight, cross_bias):
    layers, depth, share = v_weight.shape
    rank = share * lax.axis_size("dp")
    rows = features.shape[0] // CHUNKS
    late = rows - EARLY
    quarter = rank // 4
    tasks = layers * CHUNKS
    dma = pltpu.SemaphoreType.DMA
    anywhere = pl.BlockSpec(memory_space=pltpu.HBM)
    arguments = [
        pltpu.with_memory_space_constraint(array, pltpu.HBM)
        for array in (features, jnp.swapaxes(v_weight, 1, 2), u_weight, cross_bias)
    ]
    return pl.pallas_call(
        kernel,
        out_shape=jax.ShapeDtypeStruct(features.shape, BF16),
        in_specs=[anywhere] * 4,
        out_specs=pl.BlockSpec(memory_space=pltpu.VMEM),
        scratch_shapes=[
            pltpu.VMEM(features.shape, BF16),
            pltpu.VMEM((2 * layers, rank, depth), BF16),
            pltpu.VMEM((CHUNKS, rows, depth), BF16),
            pltpu.VMEM(cross_bias.shape, F32),
            pltpu.VMEM((tasks, 4, late, quarter), BF16),
            pltpu.VMEM((tasks, late, quarter), BF16),
            pltpu.VMEM((tasks, late, quarter), BF16),
            pltpu.VMEM((tasks, 2, late, quarter), BF16),
            pltpu.VMEM((tasks, late, quarter), BF16),
            pltpu.VMEM((tasks, late, quarter), BF16),
            pltpu.VMEM((tasks, 4, late, quarter), BF16),
            pltpu.VMEM((tasks, 2, 4, EARLY, quarter // 2), BF16),
            pltpu.VMEM((tasks, 4, EARLY, quarter // 2), BF16),
            pltpu.VMEM((tasks, 4, EARLY, quarter // 2), BF16),
            pltpu.VMEM((tasks, EARLY, quarter // 2), BF16),
            pltpu.VMEM((tasks, EARLY, quarter // 2), BF16),
            pltpu.VMEM((tasks, 2, EARLY, quarter // 2), BF16),
            pltpu.VMEM((tasks, 2, 4, EARLY, quarter // 2), BF16),
            dma((11,)),
            dma((SLOTS, 11)),
            dma,
            dma((2 * layers, 5)),
            dma((3, PARTS)),
            dma((3,)),
            dma((2 * layers,)),
        ],
        compiler_params=pltpu.CompilerParams(
            collective_id=0, has_side_effects=True, vmem_limit_bytes=50 << 20
        ),
    )(*arguments)


def solution(mesh):
    return jax.shard_map(
        local,
        mesh=mesh,
        in_specs=(P("dp", "mp"), P(None, "mp", "dp"), P(None, "dp", "mp"), P(None, "mp")),
        out_specs=P("dp", "mp"),
        check_vma=False,
    )
```

```python
import jax
import jax.numpy as jnp
from jax import lax
from jax.experimental import pallas as pl
from jax.experimental.pallas import tpu as pltpu
from jax.sharding import PartitionSpec as P

MESH = pl.DeviceIdType.MESH
BF16 = jnp.bfloat16
F32 = jnp.float32

CHUNKS = 8
LAG = (0, 1, 2, 3, 4, 5, 7)
WLAG = (0, 2, 4, 6, 8)
EARLY = 64
UPPER_A, UPPER_B = 32, 32
SLOTS = 8
PARTS = 4
DIRECT = 2


def kernel(
    f_hbm, v_hbm, u_hbm, b_hbm, out_ref,
    features, w_full, carried, bias,
    part_b, far_b, mid_b, near_b, sum_b, across_b, rank_b,
    part_a, across_a, sum_a, far_a, mid_a, near_a, rank_a,
    part_d, from_d, sum_d, across_d, rank_d,
    ss, rs, wss, wrs, v0s, in_sem, own_sem, sd, rd,
):
    layers = v_hbm.shape[0]
    matrices = 2 * layers
    rows = f_hbm.shape[0] // CHUNKS
    late = rows - EARLY
    depth = f_hbm.shape[1]
    share = u_hbm.shape[1]
    block_width = 2 * share
    tasks = layers * CHUNKS
    quarter = w_full.shape[1] // 4

    dp, mp = lax.axis_index("dp"), lax.axis_index("mp")
    y_hi, z, core = dp // 8, lax.rem(dp // 2, 4), lax.rem(dp, 2)
    y_lo, x = mp // 4, lax.rem(mp, 4)
    xr, xl, xo = lax.rem(x + 1, 4), lax.rem(x + 3, 4), lax.rem(x + 2, 4)
    zr, zl, zo = lax.rem(z + 1, 4), lax.rem(z + 3, 4), lax.rem(z + 2, 4)

    def at(y_hi=y_hi, z=z, core=core, y_lo=y_lo, x=x):
        return ((y_hi * 4 + z) * 2 + core, y_lo * 4 + x)

    right, left, opposite, across = at(x=xr), at(x=xl), at(x=xo), at(y_lo=1 - y_lo)
    z_right, z_left, y_far, partner = at(z=zr), at(z=zl), at(y_hi=1 - y_hi), at(core=1 - core)

    barrier = pltpu.get_barrier_semaphore()
    for device in (right, left, opposite, across, z_right, z_left, y_far, partner):
        pl.semaphore_signal(barrier, inc=1, device_id=device, device_id_type=MESH)

    def send(src, dst, send_sem, recv_sem, device):
        return pltpu.make_async_remote_copy(
            src_ref=src, dst_ref=dst, send_sem=send_sem, recv_sem=recv_sem,
            device_id=device, device_id_type=MESH,
        )

    def start(copies):
        for copy in copies:
            copy.start()

    own, same, other = y_hi * 4 + z, y_hi * 4, (1 - y_hi) * 4

    def piece(matrix, block):
        first = pl.multiple_of(block * block_width + core * share, share)
        return w_full.at[matrix, pl.ds(first, share), :]

    def move(matrix, block, number, device):
        place = piece(matrix, block)
        return send(place, place, wss, wrs.at[matrix, number], device)

    def arrived(matrix, number, pieces):
        place = w_full.at[matrix, pl.ds(0, pieces * share), :]
        send(place, place, wss, wrs.at[matrix, number], partner).wait_recv()

    def own_piece(matrix):
        source = v_hbm if matrix % 2 == 0 else u_hbm
        return pltpu.make_async_copy(source.at[matrix // 2], piece(matrix, own), own_sem.at[matrix])

    def weights_0(matrix):
        start([move(matrix, own, 1, z_right), move(matrix, own, 1, z_left), move(matrix, own, 4, partner)])

    def weights_1(matrix):
        arrived(matrix, 1, 2)
        start([move(matrix, same + zl, 3, z_right), move(matrix, same + zl, 4, partner),
               move(matrix, same + zr, 4, partner)])
        arrived(matrix, 0, 1)
        start([move(matrix, other + z, 2, z_right), move(matrix, other + z, 2, z_left),
               move(matrix, other + z, 4, partner)])

    def weights_2(matrix):
        arrived(matrix, 2, 2)
        start([move(matrix, other + zr, 3, z_left), move(matrix, other + zl, 4, partner),
               move(matrix, other + zr, 4, partner)])

    def weights_3(matrix):
        arrived(matrix, 3, 2)
        start([move(matrix, same + zo, 4, partner), move(matrix, other + zo, 4, partner)])

    def weights_4(matrix):
        arrived(matrix, 4, 8)

    weight_stages = (weights_0, weights_1, weights_2, weights_3, weights_4)
    weight_sends = 4 + 6 + 3 + 2

    def down_0():
        step = share // PARTS

        def sub(block, s, sem, device):
            first = pl.multiple_of(block * block_width + core * share + s * step, step)
            place = w_full.at[0, pl.ds(first, step), :]
            return send(place, place, wss, sem, device)

        def landed(kind, s):
            sub(own, s, v0s.at[kind, s], partner).wait_recv()

        for s in range(PARTS):
            start([sub(own, s, v0s.at[0, s], z_right), sub(own, s, wrs.at[0, 0], z_left), sub(own, s, v0s.at[1, s], y_far)])
        move(0, own, 4, partner).start()
        for matrix in range(1, matrices):
            move(matrix, own, 0, y_far).start()
        for s in range(PARTS):
            landed(0, s)
            sub(same + zl, s, wrs.at[0, 2], z_right).start()
            landed(1, s)
            start([sub(other + z, s, wrs.at[0, 1], z_right), sub(other + z, s, v0s.at[2, s], z_left)])
        start([move(0, same + zl, 4, partner), move(0, other + z, 4, partner)])
        arrived(0, 0, 1)
        move(0, same + zr, 4, partner).start()
        for s in range(PARTS):
            landed(2, s)
            sub(other + zr, s, wrs.at[0, 3], z_left).start()
        move(0, other + zr, 4, partner).start()
        arrived(0, 1, 1)
        move(0, other + zl, 4, partner).start()
        weights_0(1)
        arrived(0, 2, 1)
        move(0, same + zo, 4, partner).start()
        arrived(0, 3, 1)
        move(0, other + zo, 4, partner).start()
        arrived(0, 4, 8)

    def to_right_and_left(t, rows, upper, part, far, mid, near, rank, first):
        upper, lower = pl.ds(0, upper), pl.ds(upper, rows - upper)

        def hop_1():
            start([
                send(part(xo).at[upper], far.at[t, upper], ss.at[first], rs.at[lax.rem(t, SLOTS), first], right),
                send(part(xo).at[lower], far.at[t, lower], ss.at[first], rs.at[lax.rem(t, SLOTS), first], left),
                send(part(xr).at[lower], near.at[t, 0, lower], ss.at[first], rs.at[lax.rem(t, SLOTS), first + 1], right),
                send(part(xl).at[upper], near.at[t, 0, upper], ss.at[first], rs.at[lax.rem(t, SLOTS), first + 1], left),
            ])

        def hop_2():
            await_recv(t, first, far)
            mid[t, upper] = (part(xr)[upper].astype(F32) + far[t, upper].astype(F32)).astype(BF16)
            mid[t, lower] = (part(xl)[lower].astype(F32) + far[t, lower].astype(F32)).astype(BF16)
            start([
                send(mid.at[t, upper], near.at[t, 1, upper], ss.at[first + 1], rs.at[lax.rem(t, SLOTS), first + 1], right),
                send(mid.at[t, lower], near.at[t, 1, lower], ss.at[first + 1], rs.at[lax.rem(t, SLOTS), first + 1], left),
            ])

        def total():
            await_recv(t, first + 1, near)
            return (
                part(x)[...].astype(F32) + near[t, 0].astype(F32) + near[t, 1].astype(F32)
            ).astype(BF16)

        def share_1():
            start([
                send(rank(x), rank(x), ss.at[first + 2], rs.at[lax.rem(t, SLOTS), first + 2], right),
                send(rank(x), rank(x), ss.at[first + 2], rs.at[lax.rem(t, SLOTS), first + 2], left),
            ])

        def share_2():
            await_recv(t, first + 2, near)
            start([
                send(rank(xl).at[lower], rank(xl).at[lower], ss.at[first + 3], rs.at[lax.rem(t, SLOTS), first + 3], right),
                send(rank(xr).at[upper], rank(xr).at[upper], ss.at[first + 3], rs.at[lax.rem(t, SLOTS), first + 3], left),
            ])

        return hop_1, hop_2, total, share_1, share_2

    def ways(t):
        late_ways = to_right_and_left(
            t, late, UPPER_B, lambda q: part_b.at[t, q], far_b, mid_b, near_b, lambda q: rank_b.at[t, q], 0
        )
        early_ways = to_right_and_left(
            t, EARLY, UPPER_A, lambda q: sum_a.at[t, q], far_a, mid_a, near_a, lambda q: rank_a.at[t, y_lo, q], 4
        )
        return late_ways, early_ways

    def over_y(t, src, dst, number):
        send(src, dst, ss.at[number], rs.at[lax.rem(t, SLOTS), number], across).start()

    def await_recv(t, number, size):
        send(size.at[t], size.at[t], ss.at[0], rs.at[lax.rem(t, SLOTS), number], right).wait_recv()

    def chunk_rows(chunk):
        return pl.ds(pl.multiple_of(chunk * rows, rows), rows)

    def down(t):
        layer, chunk = t // CHUNKS, lax.rem(t, CHUNKS)
        for q in range(4):
            yield q, lax.dot_general(
                carried[chunk],
                w_full[2 * layer, q * quarter : (q + 1) * quarter, :],
                (((1,), (1,)), ((), ())),
                preferred_element_type=F32,
            ).astype(BF16)

    def up(t, lhs):
        layer, chunk = t // CHUNKS, lax.rem(t, CHUNKS)
        for j in range(4):
            columns = slice(j * depth // 4, (j + 1) * depth // 4)
            total = bias[pl.ds(layer, 1), columns]
            for q in range(4):
                total = total + jnp.dot(
                    lhs[q],
                    w_full[2 * layer + 1, q * quarter : (q + 1) * quarter, columns],
                    preferred_element_type=F32,
                )
            carried[chunk, :, columns] = (
                features[chunk_rows(chunk), columns].astype(F32) * total + carried[chunk, :, columns].astype(F32)
            ).astype(BF16)

        @pl.when(layer == layers - 1)
        def _():
            out_ref[chunk_rows(chunk), :] = carried[chunk]

    def stage_0(t):
        for q, value in down(t):
            part_b[t, q] = value[:late]
            part_a[t, 0, q] = value[late:, : quarter // 2]
            part_a[t, 1, q] = value[late:, quarter // 2 :]
        over_y(t, part_a.at[t, 1 - y_lo], across_a.at[t], 9)
        ways(t)[0][0]()

    def stage_1(t):
        late_ways, early_ways = ways(t)
        await_recv(t, 9, across_a)
        sum_a[t] = (part_a[t, y_lo].astype(F32) + across_a[t].astype(F32)).astype(BF16)
        early_ways[0]()
        late_ways[1]()

    def stage_2(t):
        late_ways, early_ways = ways(t)
        early_ways[1]()
        sum_b[t] = late_ways[2]()
        over_y(t, sum_b.at[t], across_b.at[t], 8)

    def stage_3(t):
        late_ways, early_ways = ways(t)
        rank_a[t, y_lo, x] = early_ways[2]()
        early_ways[3]()
        await_recv(t, 8, across_b)
        rank_b[t, x] = (sum_b[t].astype(F32) + across_b[t].astype(F32)).astype(BF16)
        late_ways[3]()

    def stage_4(t):
        late_ways, early_ways = ways(t)
        early_ways[4]()
        late_ways[4]()

    def stage_5(t):
        await_recv(t, 7, far_a)
        over_y(t, rank_a.at[t, y_lo], rank_a.at[t, y_lo], 10)

    def stage_6(t):
        await_recv(t, 3, far_b)
        await_recv(t, 10, across_a)
        up(t, [
            jnp.concatenate(
                [rank_b[t, q], jnp.concatenate([rank_a[t, 0, q], rank_a[t, 1, q]], axis=1)], axis=0
            )
            for q in range(4)
        ])

    def await_direct(n, number, size):
        send(size, size, sd.at[0], rd.at[n, number], right).wait_recv()

    def direct_0(t):
        n = t - direct_from
        for q, value in down(t):
            part_d[n, q] = value
        start([
            send(part_d.at[n, xo], from_d.at[n, 2], sd.at[0], rd.at[n, 0], opposite),
            send(part_d.at[n, xr], from_d.at[n, 0], sd.at[0], rd.at[n, 0], right),
            send(part_d.at[n, xl], from_d.at[n, 1], sd.at[0], rd.at[n, 0], left),
        ])

    def direct_1(t):
        n = t - direct_from
        await_direct(n, 0, from_d.at[n])
        sum_d[n] = (
            part_d[n, x].astype(F32)
            + from_d[n, 0].astype(F32)
            + from_d[n, 1].astype(F32)
            + from_d[n, 2].astype(F32)
        ).astype(BF16)
        send(sum_d.at[n], across_d.at[n], sd.at[1], rd.at[n, 1], across).start()

    def direct_2(t):
        n = t - direct_from
        await_direct(n, 1, across_d.at[n])
        rank_d[n, x] = (sum_d[n].astype(F32) + across_d[n].astype(F32)).astype(BF16)
        start([
            send(rank_d.at[n, x], rank_d.at[n, x], sd.at[2], rd.at[n, 2], device)
            for device in (opposite, right, left)
        ])

    def direct_3(t):
        n = t - direct_from
        await_direct(n, 2, from_d.at[n])
        up(t, [rank_d[n, q] for q in range(4)])

    direct_from = tasks - DIRECT
    steps = [
        (stage_0, "s0", LAG[0], 0, direct_from), (direct_0, "d0", 0, direct_from, tasks),
        (stage_1, "s1", LAG[1], 0, direct_from), (direct_1, "d1", 1, direct_from, tasks),
        (stage_2, "s2", LAG[2], 0, direct_from), (direct_2, "d2", 2, direct_from, tasks),
        (stage_3, "s3", LAG[3], 0, direct_from), (stage_4, "s4", LAG[4], 0, direct_from),
        (stage_5, "s5", LAG[5], 0, direct_from), (stage_6, "s6", LAG[6], 0, direct_from),
        (direct_3, "d3", 3, direct_from, tasks),
    ]

    for matrix in range(matrices):
        own_piece(matrix).start()
    fetches = [pltpu.make_async_copy(f_hbm, features, in_sem.at[0]), pltpu.make_async_copy(b_hbm, bias, in_sem.at[2])] + [
        pltpu.make_async_copy(f_hbm.at[pl.ds(chunk * rows, rows), :], carried.at[chunk], in_sem.at[1])
        for chunk in range(CHUNKS)
    ]
    start(fetches)
    with jax.named_scope("barrier"):
        pl.semaphore_wait(barrier, 8)
    with jax.named_scope("fetch"):
        for matrix in range(matrices):
            own_piece(matrix).wait()
    with jax.named_scope("v0"):
        down_0()
    with jax.named_scope("v0c"):
        for fetch in fetches:
            fetch.wait()

    def weights_at(i, number):
        turn = i - WLAG[number]
        first = turn == -WLAG[1]
        matrix = jnp.where(first, 1, turn // 4 + 2)
        regular = jnp.logical_and(jnp.logical_and(turn >= 0, lax.rem(turn, 4) == 0), matrix < matrices)

        @pl.when(jnp.logical_or(first, regular))
        def _():
            with jax.named_scope(f"w{number}"):
                weight_stages[number](matrix)

    @pl.loop(0, max(direct_from + LAG[6], tasks + 3))
    def _(i):
        weights_at(i, 4)
        for stage, name, lag, first, end in steps:
            t = i - lag

            @pl.when(jnp.logical_and(t >= first, t < end))
            def _(stage=stage, name=name, t=t):
                with jax.named_scope(name):
                    stage(t)

        for number in range(4):
            weights_at(i, number)

    with jax.named_scope("end"):
        sent = (
            near_b, far_b, near_b, far_b, near_a, far_a, near_a, far_a, across_b, across_a, across_a
        )
        for number, size in enumerate(sent):
            send(size, size, ss.at[number], rs.at[0, 0], right).wait_send()
        for number, size in enumerate((from_d, across_d, from_d)):
            send(size, size, sd.at[number], rd.at[0, 0], right).wait_send()
        for matrix in range(matrices):
            place = w_full.at[matrix, pl.ds(0, weight_sends * share), :]
            send(place, place, wss, wrs.at[0, 0], right).wait_send()


def local(features, v_weight, u_weight, cross_bias):
    layers, depth, share = v_weight.shape
    rank = share * lax.axis_size("dp")
    rows = features.shape[0] // CHUNKS
    late = rows - EARLY
    quarter = rank // 4
    tasks = layers * CHUNKS - DIRECT
    dma = pltpu.SemaphoreType.DMA
    anywhere = pl.BlockSpec(memory_space=pltpu.HBM)
    arguments = [
        pltpu.with_memory_space_constraint(array, pltpu.HBM)
        for array in (features, jnp.swapaxes(v_weight, 1, 2), u_weight, cross_bias)
    ]
    return pl.pallas_call(
        kernel,
        out_shape=jax.ShapeDtypeStruct(features.shape, BF16),
        in_specs=[anywhere] * 4,
        out_specs=pl.BlockSpec(memory_space=pltpu.VMEM),
        scratch_shapes=[
            pltpu.VMEM(features.shape, BF16),
            pltpu.VMEM((2 * layers, rank, depth), BF16),
            pltpu.VMEM((CHUNKS, rows, depth), BF16),
            pltpu.VMEM(cross_bias.shape, F32),
            pltpu.VMEM((tasks, 4, late, quarter), BF16),
            pltpu.VMEM((tasks, late, quarter), BF16),
            pltpu.VMEM((tasks, late, quarter), BF16),
            pltpu.VMEM((tasks, 2, late, quarter), BF16),
            pltpu.VMEM((tasks, late, quarter), BF16),
            pltpu.VMEM((tasks, late, quarter), BF16),
            pltpu.VMEM((tasks, 4, late, quarter), BF16),
            pltpu.VMEM((tasks, 2, 4, EARLY, quarter // 2), BF16),
            pltpu.VMEM((tasks, 4, EARLY, quarter // 2), BF16),
            pltpu.VMEM((tasks, 4, EARLY, quarter // 2), BF16),
            pltpu.VMEM((tasks, EARLY, quarter // 2), BF16),
            pltpu.VMEM((tasks, EARLY, quarter // 2), BF16),
            pltpu.VMEM((tasks, 2, EARLY, quarter // 2), BF16),
            pltpu.VMEM((tasks, 2, 4, EARLY, quarter // 2), BF16),
            pltpu.VMEM((DIRECT, 4, rows, quarter), BF16),
            pltpu.VMEM((DIRECT, 3, rows, quarter), BF16),
            pltpu.VMEM((DIRECT, rows, quarter), BF16),
            pltpu.VMEM((DIRECT, rows, quarter), BF16),
            pltpu.VMEM((DIRECT, 4, rows, quarter), BF16),
            dma((11,)),
            dma((SLOTS, 11)),
            dma,
            dma((2 * layers, 5)),
            dma((3, PARTS)),
            dma((3,)),
            dma((2 * layers,)),
            dma((3,)),
            dma((DIRECT, 3)),
        ],
        compiler_params=pltpu.CompilerParams(
            collective_id=0, has_side_effects=True, vmem_limit_bytes=50 << 20
        ),
    )(*arguments)


def solution(mesh):
    return jax.shard_map(
        local,
        mesh=mesh,
        in_specs=(P("dp", "mp"), P(None, "mp", "dp"), P(None, "dp", "mp"), P(None, "mp")),
        out_specs=P("dp", "mp"),
        check_vma=False,
    )
```

```python
import jax
import jax.numpy as jnp
from jax import lax
from jax.experimental import pallas as pl
from jax.experimental.pallas import tpu as pltpu
from jax.sharding import PartitionSpec as P

MESH = pl.DeviceIdType.MESH
BF16 = jnp.bfloat16
F32 = jnp.float32

CHUNKS = 8
LAGS = {"a1": 1, "a2": 2, "a3": 3, "a4": 4, "a5": 5, "b1": 1, "b2": 2, "b3": 3, "b4": 4, "up": 7}
ORDER = ("down", "a1", "b1", "a2", "b2", "a3", "b3", "a4", "b4", "a5", "up")
WLAG = (0, 3, 5, 8)
WFIRST = -1
EARLY = 64
UPPER_A, UPPER_B = 32, 32
SLOTS = 8
PARTS = 4
DIRECT = 2
DLAG = (0, 1, 2, 5)


def kernel(
    f_hbm, v_hbm, u_hbm, b_hbm, out_ref,
    features, w_full, carried, bias,
    part_b, far_b, mid_b, near_b, sum_b, across_b, rank_b,
    part_a, across_a, sum_a, far_a, mid_a, near_a, rank_a,
    part_d, from_d, sum_d, across_d, rank_d,
    ss, rs, wss, wrs, v0s, in_sem, own_sem, sd, rd,
):
    layers = v_hbm.shape[0]
    matrices = 2 * layers
    rows = f_hbm.shape[0] // CHUNKS
    late = rows - EARLY
    depth = f_hbm.shape[1]
    share = u_hbm.shape[1]
    block_width = 2 * share
    tasks = layers * CHUNKS
    quarter = w_full.shape[1] // 4

    dp, mp = lax.axis_index("dp"), lax.axis_index("mp")
    y_hi, z, core = dp // 8, lax.rem(dp // 2, 4), lax.rem(dp, 2)
    y_lo, x = mp // 4, lax.rem(mp, 4)
    xr, xl, xo = lax.rem(x + 1, 4), lax.rem(x + 3, 4), lax.rem(x + 2, 4)
    zr, zl, zo = lax.rem(z + 1, 4), lax.rem(z + 3, 4), lax.rem(z + 2, 4)

    def at(y_hi=y_hi, z=z, core=core, y_lo=y_lo, x=x):
        return ((y_hi * 4 + z) * 2 + core, y_lo * 4 + x)

    right, left, opposite, across = at(x=xr), at(x=xl), at(x=xo), at(y_lo=1 - y_lo)
    z_right, z_left, y_far, partner = at(z=zr), at(z=zl), at(y_hi=1 - y_hi), at(core=1 - core)

    barrier = pltpu.get_barrier_semaphore()
    for device in (right, left, opposite, across, z_right, z_left, y_far, partner):
        pl.semaphore_signal(barrier, inc=1, device_id=device, device_id_type=MESH)

    def send(src, dst, send_sem, recv_sem, device):
        return pltpu.make_async_remote_copy(
            src_ref=src, dst_ref=dst, send_sem=send_sem, recv_sem=recv_sem,
            device_id=device, device_id_type=MESH,
        )

    def start(copies):
        for copy in copies:
            copy.start()

    own, same, other = y_hi * 4 + z, y_hi * 4, (1 - y_hi) * 4

    def piece(matrix, block):
        first = pl.multiple_of(block * block_width + core * share, share)
        return w_full.at[matrix, pl.ds(first, share), :]

    def move(matrix, block, number, device):
        place = piece(matrix, block)
        return send(place, place, wss, wrs.at[matrix, number], device)

    def arrived(matrix, number, pieces):
        place = w_full.at[matrix, pl.ds(0, pieces * share), :]
        send(place, place, wss, wrs.at[matrix, number], partner).wait_recv()

    def own_piece(matrix):
        source = v_hbm if matrix % 2 == 0 else u_hbm
        return pltpu.make_async_copy(source.at[matrix // 2], piece(matrix, own), own_sem.at[matrix])

    def weights_0(matrix):
        start([move(matrix, own, 1, z_right), move(matrix, own, 1, z_left), move(matrix, own, 4, partner)])
        arrived(matrix, 0, 1)
        start([move(matrix, other + z, 2, z_right), move(matrix, other + z, 2, z_left),
               move(matrix, other + z, 4, partner)])

    def weights_1(matrix):
        arrived(matrix, 1, 2)
        start([move(matrix, same + zl, 3, z_right), move(matrix, same + zl, 4, partner),
               move(matrix, same + zr, 4, partner)])
        arrived(matrix, 2, 2)
        start([move(matrix, other + zr, 3, z_left), move(matrix, other + zl, 4, partner),
               move(matrix, other + zr, 4, partner)])

    def weights_2(matrix):
        arrived(matrix, 3, 2)
        start([move(matrix, same + zo, 4, partner), move(matrix, other + zo, 4, partner)])

    def weights_3(matrix):
        arrived(matrix, 4, 8)

    weight_stages = (weights_0, weights_1, weights_2, weights_3)
    weight_sends = 4 + 6 + 3 + 2

    def down_0():
        step = share // PARTS

        def sub(block, s, sem, device):
            first = pl.multiple_of(block * block_width + core * share + s * step, step)
            place = w_full.at[0, pl.ds(first, step), :]
            return send(place, place, wss, sem, device)

        def landed(kind, s):
            sub(own, s, v0s.at[kind, s], partner).wait_recv()

        for s in range(PARTS):
            start([sub(own, s, v0s.at[0, s], z_right), sub(own, s, wrs.at[0, 0], z_left), sub(own, s, v0s.at[1, s], y_far)])
        move(0, own, 4, partner).start()
        for matrix in range(1, matrices):
            move(matrix, own, 0, y_far).start()
        for s in range(PARTS):
            landed(0, s)
            sub(same + zl, s, wrs.at[0, 2], z_right).start()
            landed(1, s)
            start([sub(other + z, s, wrs.at[0, 1], z_right), sub(other + z, s, v0s.at[2, s], z_left)])
        start([move(0, same + zl, 4, partner), move(0, other + z, 4, partner)])
        arrived(0, 0, 1)
        move(0, same + zr, 4, partner).start()
        for s in range(PARTS):
            landed(2, s)
            sub(other + zr, s, wrs.at[0, 3], z_left).start()
        move(0, other + zr, 4, partner).start()
        arrived(0, 1, 1)
        move(0, other + zl, 4, partner).start()
        weights_0(1)
        arrived(0, 2, 1)
        move(0, same + zo, 4, partner).start()
        arrived(0, 3, 1)
        move(0, other + zo, 4, partner).start()
        arrived(0, 4, 8)

    def to_right_and_left(t, rows, upper, part, far, mid, near, rank, first):
        upper, lower = pl.ds(0, upper), pl.ds(upper, rows - upper)

        def hop_1():
            start([
                send(part(xo).at[upper], far.at[t, upper], ss.at[first], rs.at[lax.rem(t, SLOTS), first], right),
                send(part(xo).at[lower], far.at[t, lower], ss.at[first], rs.at[lax.rem(t, SLOTS), first], left),
                send(part(xr).at[lower], near.at[t, 0, lower], ss.at[first], rs.at[lax.rem(t, SLOTS), first + 1], right),
                send(part(xl).at[upper], near.at[t, 0, upper], ss.at[first], rs.at[lax.rem(t, SLOTS), first + 1], left),
            ])

        def hop_2():
            await_recv(t, first, far)
            mid[t, upper] = (part(xr)[upper].astype(F32) + far[t, upper].astype(F32)).astype(BF16)
            mid[t, lower] = (part(xl)[lower].astype(F32) + far[t, lower].astype(F32)).astype(BF16)
            start([
                send(mid.at[t, upper], near.at[t, 1, upper], ss.at[first + 1], rs.at[lax.rem(t, SLOTS), first + 1], right),
                send(mid.at[t, lower], near.at[t, 1, lower], ss.at[first + 1], rs.at[lax.rem(t, SLOTS), first + 1], left),
            ])

        def total():
            await_recv(t, first + 1, near)
            return (
                part(x)[...].astype(F32) + near[t, 0].astype(F32) + near[t, 1].astype(F32)
            ).astype(BF16)

        def share_1():
            start([
                send(rank(x), rank(x), ss.at[first + 2], rs.at[lax.rem(t, SLOTS), first + 2], right),
                send(rank(x), rank(x), ss.at[first + 2], rs.at[lax.rem(t, SLOTS), first + 2], left),
            ])

        def share_2():
            await_recv(t, first + 2, near)
            start([
                send(rank(xl).at[lower], rank(xl).at[lower], ss.at[first + 3], rs.at[lax.rem(t, SLOTS), first + 3], right),
                send(rank(xr).at[upper], rank(xr).at[upper], ss.at[first + 3], rs.at[lax.rem(t, SLOTS), first + 3], left),
            ])

        return hop_1, hop_2, total, share_1, share_2

    def ways(t):
        late_ways = to_right_and_left(
            t, late, UPPER_B, lambda q: part_b.at[t, q], far_b, mid_b, near_b, lambda q: rank_b.at[t, q], 0
        )
        early_ways = to_right_and_left(
            t, EARLY, UPPER_A, lambda q: sum_a.at[t, q], far_a, mid_a, near_a, lambda q: rank_a.at[t, y_lo, q], 4
        )
        return late_ways, early_ways

    def over_y(t, src, dst, number):
        send(src, dst, ss.at[number], rs.at[lax.rem(t, SLOTS), number], across).start()

    def await_recv(t, number, size):
        send(size.at[t], size.at[t], ss.at[0], rs.at[lax.rem(t, SLOTS), number], right).wait_recv()

    def chunk_rows(chunk):
        return pl.ds(pl.multiple_of(chunk * rows, rows), rows)

    def down(t):
        layer, chunk = t // CHUNKS, lax.rem(t, CHUNKS)
        for q in range(4):
            yield q, lax.dot_general(
                carried[chunk],
                w_full[2 * layer, q * quarter : (q + 1) * quarter, :],
                (((1,), (1,)), ((), ())),
                preferred_element_type=F32,
            ).astype(BF16)

    def up(t, lhs):
        layer, chunk = t // CHUNKS, lax.rem(t, CHUNKS)
        for j in range(4):
            columns = slice(j * depth // 4, (j + 1) * depth // 4)
            total = bias[pl.ds(layer, 1), columns]
            for q in range(4):
                total = total + jnp.dot(
                    lhs[q],
                    w_full[2 * layer + 1, q * quarter : (q + 1) * quarter, columns],
                    preferred_element_type=F32,
                )
            carried[chunk, :, columns] = (
                features[chunk_rows(chunk), columns].astype(F32) * total + carried[chunk, :, columns].astype(F32)
            ).astype(BF16)

        @pl.when(layer == layers - 1)
        def _():
            out_ref[chunk_rows(chunk), :] = carried[chunk]

    def stage_0(t):
        for q, value in down(t):
            part_b[t, q] = value[:late]
            part_a[t, 0, q] = value[late:, : quarter // 2]
            part_a[t, 1, q] = value[late:, quarter // 2 :]
        over_y(t, part_a.at[t, 1 - y_lo], across_a.at[t], 9)
        ways(t)[0][0]()

    def early_1(t):
        await_recv(t, 9, across_a)
        sum_a[t] = (part_a[t, y_lo].astype(F32) + across_a[t].astype(F32)).astype(BF16)
        ways(t)[1][0]()

    def early_2(t):
        ways(t)[1][1]()

    def early_3(t):
        early_ways = ways(t)[1]
        rank_a[t, y_lo, x] = early_ways[2]()
        early_ways[3]()

    def early_4(t):
        ways(t)[1][4]()

    def early_5(t):
        await_recv(t, 7, far_a)
        over_y(t, rank_a.at[t, y_lo], rank_a.at[t, y_lo], 10)

    def late_1(t):
        ways(t)[0][1]()

    def late_2(t):
        sum_b[t] = ways(t)[0][2]()
        over_y(t, sum_b.at[t], across_b.at[t], 8)

    def late_3(t):
        await_recv(t, 8, across_b)
        rank_b[t, x] = (sum_b[t].astype(F32) + across_b[t].astype(F32)).astype(BF16)
        ways(t)[0][3]()

    def late_4(t):
        ways(t)[0][4]()

    def stage_6(t):
        await_recv(t, 3, far_b)
        await_recv(t, 10, across_a)
        up(t, [
            jnp.concatenate(
                [rank_b[t, q], jnp.concatenate([rank_a[t, 0, q], rank_a[t, 1, q]], axis=1)], axis=0
            )
            for q in range(4)
        ])

    def await_direct(n, number, size):
        send(size, size, sd.at[0], rd.at[n, number], right).wait_recv()

    def direct_0(t):
        n = t - direct_from
        for q, value in down(t):
            part_d[n, q] = value
        start([
            send(part_d.at[n, xo], from_d.at[n, 2], sd.at[0], rd.at[n, 0], opposite),
            send(part_d.at[n, xr], from_d.at[n, 0], sd.at[0], rd.at[n, 0], right),
            send(part_d.at[n, xl], from_d.at[n, 1], sd.at[0], rd.at[n, 0], left),
        ])

    def direct_1(t):
        n = t - direct_from
        await_direct(n, 0, from_d.at[n])
        sum_d[n] = (
            part_d[n, x].astype(F32)
            + from_d[n, 0].astype(F32)
            + from_d[n, 1].astype(F32)
            + from_d[n, 2].astype(F32)
        ).astype(BF16)
        send(sum_d.at[n], across_d.at[n], sd.at[1], rd.at[n, 1], across).start()

    def direct_2(t):
        n = t - direct_from
        await_direct(n, 1, across_d.at[n])
        rank_d[n, x] = (sum_d[n].astype(F32) + across_d[n].astype(F32)).astype(BF16)
        start([
            send(rank_d.at[n, x], rank_d.at[n, x], sd.at[2], rd.at[n, 2], device)
            for device in (opposite, right, left)
        ])

    def direct_3(t):
        n = t - direct_from
        await_direct(n, 2, from_d.at[n])
        up(t, [rank_d[n, q] for q in range(4)])

    direct_from = tasks - DIRECT
    normal = {
        "a1": early_1, "a2": early_2, "a3": early_3, "a4": early_4, "a5": early_5,
        "b1": late_1, "b2": late_2, "b3": late_3, "b4": late_4, "up": stage_6,
    }
    steps = []
    for name in ORDER:
        if name == "down":
            steps += [(stage_0, name, 0, 0, direct_from), (direct_0, "d0", 0, direct_from, tasks)]
        else:
            steps.append((normal[name], name, LAGS[name], 0, direct_from))
    for stage, number in ((direct_1, 1), (direct_2, 2), (direct_3, 3)):
        steps.append((stage, f"d{number}", DLAG[number], direct_from, tasks))

    for matrix in range(matrices):
        own_piece(matrix).start()
    fetches = [pltpu.make_async_copy(f_hbm, features, in_sem.at[0]), pltpu.make_async_copy(b_hbm, bias, in_sem.at[2])] + [
        pltpu.make_async_copy(f_hbm.at[pl.ds(chunk * rows, rows), :], carried.at[chunk], in_sem.at[1])
        for chunk in range(CHUNKS)
    ]
    start(fetches)
    with jax.named_scope("barrier"):
        pl.semaphore_wait(barrier, 8)
    with jax.named_scope("fetch"):
        for matrix in range(matrices):
            own_piece(matrix).wait()
    with jax.named_scope("v0"):
        down_0()
    with jax.named_scope("v0c"):
        for fetch in fetches:
            fetch.wait()

    def weights_at(i, number):
        turn = i - WLAG[number]
        first = turn == WFIRST
        matrix = jnp.where(first, 1, turn // 4 + 2)
        regular = jnp.logical_and(jnp.logical_and(turn >= 0, lax.rem(turn, 4) == 0), matrix < matrices)

        @pl.when(jnp.logical_or(first, regular))
        def _():
            with jax.named_scope(f"w{number}"):
                weight_stages[number](matrix)

    @pl.loop(0, max(direct_from + LAGS["up"], tasks + DLAG[3]))
    def _(i):
        weights_at(i, 3)
        for stage, name, lag, first, end in steps:
            t = i - lag

            @pl.when(jnp.logical_and(t >= first, t < end))
            def _(stage=stage, name=name, t=t):
                with jax.named_scope(name):
                    stage(t)

        for number in range(3):
            weights_at(i, number)

    with jax.named_scope("end"):
        sent = (
            near_b, far_b, near_b, far_b, near_a, far_a, near_a, far_a, across_b, across_a, across_a
        )
        for number, size in enumerate(sent):
            send(size, size, ss.at[number], rs.at[0, 0], right).wait_send()
        for number, size in enumerate((from_d, across_d, from_d)):
            send(size, size, sd.at[number], rd.at[0, 0], right).wait_send()
        for matrix in range(matrices):
            place = w_full.at[matrix, pl.ds(0, weight_sends * share), :]
            send(place, place, wss, wrs.at[0, 0], right).wait_send()


def local(features, v_weight, u_weight, cross_bias):
    layers, depth, share = v_weight.shape
    rank = share * lax.axis_size("dp")
    rows = features.shape[0] // CHUNKS
    late = rows - EARLY
    quarter = rank // 4
    tasks = layers * CHUNKS - DIRECT
    dma = pltpu.SemaphoreType.DMA
    anywhere = pl.BlockSpec(memory_space=pltpu.HBM)
    arguments = [
        pltpu.with_memory_space_constraint(array, pltpu.HBM)
        for array in (features, jnp.swapaxes(v_weight, 1, 2), u_weight, cross_bias)
    ]
    return pl.pallas_call(
        kernel,
        out_shape=jax.ShapeDtypeStruct(features.shape, BF16),
        in_specs=[anywhere] * 4,
        out_specs=pl.BlockSpec(memory_space=pltpu.VMEM),
        scratch_shapes=[
            pltpu.VMEM(features.shape, BF16),
            pltpu.VMEM((2 * layers, rank, depth), BF16),
            pltpu.VMEM((CHUNKS, rows, depth), BF16),
            pltpu.VMEM(cross_bias.shape, F32),
            pltpu.VMEM((tasks, 4, late, quarter), BF16),
            pltpu.VMEM((tasks, late, quarter), BF16),
            pltpu.VMEM((tasks, late, quarter), BF16),
            pltpu.VMEM((tasks, 2, late, quarter), BF16),
            pltpu.VMEM((tasks, late, quarter), BF16),
            pltpu.VMEM((tasks, late, quarter), BF16),
            pltpu.VMEM((tasks, 4, late, quarter), BF16),
            pltpu.VMEM((tasks, 2, 4, EARLY, quarter // 2), BF16),
            pltpu.VMEM((tasks, 4, EARLY, quarter // 2), BF16),
            pltpu.VMEM((tasks, 4, EARLY, quarter // 2), BF16),
            pltpu.VMEM((tasks, EARLY, quarter // 2), BF16),
            pltpu.VMEM((tasks, EARLY, quarter // 2), BF16),
            pltpu.VMEM((tasks, 2, EARLY, quarter // 2), BF16),
            pltpu.VMEM((tasks, 2, 4, EARLY, quarter // 2), BF16),
            pltpu.VMEM((DIRECT, 4, rows, quarter), BF16),
            pltpu.VMEM((DIRECT, 3, rows, quarter), BF16),
            pltpu.VMEM((DIRECT, rows, quarter), BF16),
            pltpu.VMEM((DIRECT, rows, quarter), BF16),
            pltpu.VMEM((DIRECT, 4, rows, quarter), BF16),
            dma((11,)),
            dma((SLOTS, 11)),
            dma,
            dma((2 * layers, 5)),
            dma((3, PARTS)),
            dma((3,)),
            dma((2 * layers,)),
            dma((3,)),
            dma((DIRECT, 3)),
        ],
        compiler_params=pltpu.CompilerParams(
            collective_id=0, has_side_effects=True, vmem_limit_bytes=50 << 20
        ),
    )(*arguments)


def solution(mesh):
    return jax.shard_map(
        local,
        mesh=mesh,
        in_specs=(P("dp", "mp"), P(None, "mp", "dp"), P(None, "dp", "mp"), P(None, "mp")),
        out_specs=P("dp", "mp"),
        check_vma=False,
    )
```

```python
import jax
import jax.numpy as jnp
from jax import lax
from jax.experimental import pallas as pl
from jax.experimental.pallas import tpu as pltpu
from jax.sharding import PartitionSpec as P

MESH = pl.DeviceIdType.MESH
BF16 = jnp.bfloat16
F32 = jnp.float32

CHUNKS = 8
LAGS = {"a1": 2, "a2": 3, "a3": 4, "a4": 5, "b1": 1, "b2": 2, "b3": 3, "b4": 5, "up": 7}
ORDER = ("down", "a1", "b1", "a2", "b2", "a3", "b3", "a4", "b4", "up")
WLAG = (0, 3, 5, 8)
WFIRST = -1
EARLY = 56
UPPER_A, UPPER_B = 32, 40
SLOTS = 8
PARTS = 4
DIRECT = 2
SOON = 1
EAGER = 0
DLAG = (0, 1, 2, 4)


def kernel(
    f_hbm, v_hbm, u_hbm, b_hbm, out_ref,
    features, w_full, carried, bias,
    part_b, far_b, mid_b, near_b, sum_b, across_b, rank_b,
    part_a, across_a, sum_a, far_a, near_a, rank_a,
    part_d, from_d, sum_d, across_d, rank_d,
    ss, rs, wss, wrs, v0s, in_sem, own_sem, sd, rd,
):
    layers = v_hbm.shape[0]
    matrices = 2 * layers
    rows = f_hbm.shape[0] // CHUNKS
    late = rows - EARLY
    depth = f_hbm.shape[1]
    share = u_hbm.shape[1]
    block_width = 2 * share
    tasks = layers * CHUNKS
    quarter = w_full.shape[1] // 4

    dp, mp = lax.axis_index("dp"), lax.axis_index("mp")
    y_hi, z, core = dp // 8, lax.rem(dp // 2, 4), lax.rem(dp, 2)
    y_lo, x = mp // 4, lax.rem(mp, 4)
    xr, xl, xo = lax.rem(x + 1, 4), lax.rem(x + 3, 4), lax.rem(x + 2, 4)
    zr, zl, zo = lax.rem(z + 1, 4), lax.rem(z + 3, 4), lax.rem(z + 2, 4)

    def at(y_hi=y_hi, z=z, core=core, y_lo=y_lo, x=x):
        return ((y_hi * 4 + z) * 2 + core, y_lo * 4 + x)

    right, left, opposite, across = at(x=xr), at(x=xl), at(x=xo), at(y_lo=1 - y_lo)
    z_right, z_left, y_far, partner = at(z=zr), at(z=zl), at(y_hi=1 - y_hi), at(core=1 - core)

    barrier = pltpu.get_barrier_semaphore()
    for device in (right, left, opposite, across, z_right, z_left, y_far, partner):
        pl.semaphore_signal(barrier, inc=1, device_id=device, device_id_type=MESH)

    def send(src, dst, send_sem, recv_sem, device):
        return pltpu.make_async_remote_copy(
            src_ref=src, dst_ref=dst, send_sem=send_sem, recv_sem=recv_sem,
            device_id=device, device_id_type=MESH,
        )

    def start(copies):
        for copy in copies:
            copy.start()

    own, same, other = y_hi * 4 + z, y_hi * 4, (1 - y_hi) * 4

    def piece(matrix, block):
        first = pl.multiple_of(block * block_width + core * share, share)
        return w_full.at[matrix, pl.ds(first, share), :]

    def move(matrix, block, number, device):
        place = piece(matrix, block)
        return send(place, place, wss, wrs.at[matrix, number], device)

    def arrived(matrix, number, pieces):
        place = w_full.at[matrix, pl.ds(0, pieces * share), :]
        send(place, place, wss, wrs.at[matrix, number], partner).wait_recv()

    def own_piece(matrix):
        source = v_hbm if matrix % 2 == 0 else u_hbm
        return pltpu.make_async_copy(source.at[matrix // 2], piece(matrix, own), own_sem.at[matrix])

    def weights_0(matrix):
        start([move(matrix, own, 1, z_right), move(matrix, own, 1, z_left), move(matrix, own, 4, partner)])
        arrived(matrix, 0, 1)
        start([move(matrix, other + z, 2, z_right), move(matrix, other + z, 2, z_left),
               move(matrix, other + z, 4, partner)])

    def weights_1(matrix):
        arrived(matrix, 1, 2)
        start([move(matrix, same + zl, 3, z_right), move(matrix, same + zl, 4, partner),
               move(matrix, same + zr, 4, partner)])
        arrived(matrix, 2, 2)
        start([move(matrix, other + zr, 3, z_left), move(matrix, other + zl, 4, partner),
               move(matrix, other + zr, 4, partner)])

    def weights_2(matrix):
        arrived(matrix, 3, 2)
        start([move(matrix, same + zo, 4, partner), move(matrix, other + zo, 4, partner)])

    def weights_3(matrix):
        arrived(matrix, 4, 8)

    weight_stages = (weights_0, weights_1, weights_2, weights_3)
    weight_sends = 4 + 6 + 3 + 2

    def down_0():
        step = share // PARTS

        def sub(block, s, sem, device):
            first = pl.multiple_of(block * block_width + core * share + s * step, step)
            place = w_full.at[0, pl.ds(first, step), :]
            return send(place, place, wss, sem, device)

        def landed(kind, s):
            sub(own, s, v0s.at[kind, s], partner).wait_recv()

        for s in range(PARTS):
            start([sub(own, s, v0s.at[0, s], z_right), sub(own, s, wrs.at[0, 0], z_left), sub(own, s, v0s.at[1, s], y_far)])
        move(0, own, 4, partner).start()
        for matrix in range(1, matrices):
            move(matrix, own, 0, y_far).start()
        for s in range(PARTS):
            landed(0, s)
            sub(same + zl, s, wrs.at[0, 2], z_right).start()
            landed(1, s)
            start([sub(other + z, s, wrs.at[0, 1], z_right), sub(other + z, s, v0s.at[2, s], z_left)])
        start([move(0, same + zl, 4, partner), move(0, other + z, 4, partner)])
        arrived(0, 0, 1)
        move(0, same + zr, 4, partner).start()
        for s in range(PARTS):
            landed(2, s)
            sub(other + zr, s, wrs.at[0, 3], z_left).start()
        move(0, other + zr, 4, partner).start()
        arrived(0, 1, 1)
        move(0, other + zl, 4, partner).start()
        weights_0(1)
        arrived(0, 2, 1)
        move(0, same + zo, 4, partner).start()
        arrived(0, 3, 1)
        move(0, other + zo, 4, partner).start()
        arrived(0, 4, 8)

    def to_right_and_left(t, rows, upper, part, far, mid, near, rank, first):
        upper, lower = pl.ds(0, upper), pl.ds(upper, rows - upper)

        def hop_1():
            start([
                send(part(xo).at[upper], far.at[t, upper], ss.at[first], rs.at[lax.rem(t, SLOTS), first], right),
                send(part(xo).at[lower], far.at[t, lower], ss.at[first], rs.at[lax.rem(t, SLOTS), first], left),
                send(part(xr).at[lower], near.at[t, 0, lower], ss.at[first], rs.at[lax.rem(t, SLOTS), first + 1], right),
                send(part(xl).at[upper], near.at[t, 0, upper], ss.at[first], rs.at[lax.rem(t, SLOTS), first + 1], left),
            ])

        def hop_2():
            await_recv(t, first, far)
            mid[t, upper] = (part(xr)[upper].astype(F32) + far[t, upper].astype(F32)).astype(BF16)
            mid[t, lower] = (part(xl)[lower].astype(F32) + far[t, lower].astype(F32)).astype(BF16)
            start([
                send(mid.at[t, upper], near.at[t, 1, upper], ss.at[first + 1], rs.at[lax.rem(t, SLOTS), first + 1], right),
                send(mid.at[t, lower], near.at[t, 1, lower], ss.at[first + 1], rs.at[lax.rem(t, SLOTS), first + 1], left),
            ])

        def total():
            await_recv(t, first + 1, near)
            return (
                part(x)[...].astype(F32) + near[t, 0].astype(F32) + near[t, 1].astype(F32)
            ).astype(BF16)

        def share_1():
            start([
                send(rank(x), rank(x), ss.at[first + 2], rs.at[lax.rem(t, SLOTS), first + 2], right),
                send(rank(x), rank(x), ss.at[first + 2], rs.at[lax.rem(t, SLOTS), first + 2], left),
            ])

        def share_2():
            await_recv(t, first + 2, near)
            start([
                send(rank(xl).at[lower], rank(xl).at[lower], ss.at[first + 3], rs.at[lax.rem(t, SLOTS), first + 3], right),
                send(rank(xr).at[upper], rank(xr).at[upper], ss.at[first + 3], rs.at[lax.rem(t, SLOTS), first + 3], left),
            ])

        return hop_1, hop_2, total, share_1, share_2

    def straight(t, part, far, near, rank, first):
        def hop():
            start([
                send(part(xo), far.at[t], ss.at[first + 1], rs.at[lax.rem(t, SLOTS), first], opposite),
                send(part(xr), near.at[t, 0], ss.at[first], rs.at[lax.rem(t, SLOTS), first + 1], right),
                send(part(xl), near.at[t, 1], ss.at[first], rs.at[lax.rem(t, SLOTS), first + 1], left),
            ])

        def total():
            await_recv(t, first, far)
            await_recv(t, first + 1, near)
            return (
                part(x)[...].astype(F32) + near[t, 0].astype(F32) + near[t, 1].astype(F32) + far[t].astype(F32)
            ).astype(BF16)

        upper, lower = pl.ds(0, UPPER_A), pl.ds(UPPER_A, EARLY - UPPER_A)

        def share_1():
            start([
                send(rank(x), rank(x), ss.at[first + 2], rs.at[lax.rem(t, SLOTS), first + 2], right),
                send(rank(x), rank(x), ss.at[first + 2], rs.at[lax.rem(t, SLOTS), first + 2], left),
            ])

        def share_2():
            await_recv(t, first + 2, near)
            for q, part_of, device in ((xl, lower, right), (xr, upper, left)):
                place = rank(q).at[part_of]
                send(place, place, ss.at[first + 3], rs.at[lax.rem(t, SLOTS), first + 3], device).start()

        return hop, total, share_1, share_2

    def ways(t):
        late_ways = to_right_and_left(
            t, late, UPPER_B, lambda q: part_b.at[t, q], far_b, mid_b, near_b, lambda q: rank_b.at[t, q], 0
        )
        early_ways = straight(t, lambda q: sum_a.at[t, q], far_a, near_a, lambda q: rank_a.at[t, y_lo, q], 4)
        return late_ways, early_ways

    def over_y(t, src, dst, number):
        send(src, dst, ss.at[number], rs.at[lax.rem(t, SLOTS), number], across).start()

    def await_recv(t, number, size):
        send(size.at[t], size.at[t], ss.at[0], rs.at[lax.rem(t, SLOTS), number], right).wait_recv()

    def chunk_rows(chunk):
        return pl.ds(pl.multiple_of(chunk * rows, rows), rows)

    def down(t):
        layer, chunk = t // CHUNKS, lax.rem(t, CHUNKS)
        for q in range(4):
            yield q, lax.dot_general(
                carried[chunk],
                w_full[2 * layer, q * quarter : (q + 1) * quarter, :],
                (((1,), (1,)), ((), ())),
                preferred_element_type=F32,
            ).astype(BF16)

    def up(t, lhs):
        layer, chunk = t // CHUNKS, lax.rem(t, CHUNKS)
        for j in range(4):
            columns = slice(j * depth // 4, (j + 1) * depth // 4)
            total = bias[pl.ds(layer, 1), columns]
            for q in range(4):
                total = total + jnp.dot(
                    lhs[q],
                    w_full[2 * layer + 1, q * quarter : (q + 1) * quarter, columns],
                    preferred_element_type=F32,
                )
            carried[chunk, :, columns] = (
                features[chunk_rows(chunk), columns].astype(F32) * total + carried[chunk, :, columns].astype(F32)
            ).astype(BF16)

        @pl.when(layer == layers - 1)
        def _():
            out_ref[chunk_rows(chunk), :] = carried[chunk]

    def stage_0(t):
        for q, value in down(t):
            part_b[t, q] = value[:late]
            part_a[t, 0, q] = value[late:, : quarter // 2]
            part_a[t, 1, q] = value[late:, quarter // 2 :]
        over_y(t, part_a.at[t, 1 - y_lo], across_a.at[t], 9)
        ways(t)[0][0]()

    def early_1(t):
        await_recv(t, 9, across_a)
        sum_a[t] = (part_a[t, y_lo].astype(F32) + across_a[t].astype(F32)).astype(BF16)
        ways(t)[1][0]()

    def early_2(t):
        early_ways = ways(t)[1]
        rank_a[t, y_lo, x] = early_ways[1]()
        early_ways[2]()

    def early_3(t):
        ways(t)[1][3]()

    def early_4(t):
        await_recv(t, 7, far_a)
        over_y(t, rank_a.at[t, y_lo], rank_a.at[t, y_lo], 10)

    def late_1(t):
        ways(t)[0][1]()

    def late_2(t):
        sum_b[t] = ways(t)[0][2]()
        over_y(t, sum_b.at[t], across_b.at[t], 8)

    def late_3(t):
        await_recv(t, 8, across_b)
        rank_b[t, x] = (sum_b[t].astype(F32) + across_b[t].astype(F32)).astype(BF16)
        ways(t)[0][3]()

    def late_4(t):
        ways(t)[0][4]()

    def stage_6(t):
        await_recv(t, 3, far_b)
        await_recv(t, 10, across_a)
        up(t, [
            jnp.concatenate(
                [rank_b[t, q], jnp.concatenate([rank_a[t, 0, q], rank_a[t, 1, q]], axis=1)], axis=0
            )
            for q in range(4)
        ])

    def await_direct(n, number, size):
        send(size, size, sd.at[0], rd.at[n, number], right).wait_recv()

    def direct_0(t):
        n = t - direct_from
        for q, value in down(t):
            part_d[n, q] = value
        start([
            send(part_d.at[n, xo], from_d.at[n, 2], sd.at[0], rd.at[n, 0], opposite),
            send(part_d.at[n, xr], from_d.at[n, 0], sd.at[0], rd.at[n, 0], right),
            send(part_d.at[n, xl], from_d.at[n, 1], sd.at[0], rd.at[n, 0], left),
        ])

    def direct_1(t):
        n = t - direct_from
        await_direct(n, 0, from_d.at[n])
        sum_d[n] = (
            part_d[n, x].astype(F32)
            + from_d[n, 0].astype(F32)
            + from_d[n, 1].astype(F32)
            + from_d[n, 2].astype(F32)
        ).astype(BF16)
        send(sum_d.at[n], across_d.at[n], sd.at[1], rd.at[n, 1], across).start()

    def direct_2(t):
        n = t - direct_from
        await_direct(n, 1, across_d.at[n])
        rank_d[n, x] = (sum_d[n].astype(F32) + across_d[n].astype(F32)).astype(BF16)
        start([
            send(rank_d.at[n, x], rank_d.at[n, x], sd.at[2], rd.at[n, 2], device)
            for device in (opposite, right, left)
        ])

    def direct_3(t):
        n = t - direct_from
        await_direct(n, 2, from_d.at[n])
        up(t, [rank_d[n, q] for q in range(4)])

    direct_from = tasks - DIRECT
    normal = {
        "a1": early_1, "a2": early_2, "a3": early_3, "a4": early_4,
        "b1": late_1, "b2": late_2, "b3": late_3, "b4": late_4, "up": stage_6,
    }
    steps = []
    for name in ORDER:
        if name == "down":
            steps.append((stage_0, name, 0, 0, direct_from))
        elif name == "up":
            steps.append((stage_6, name, LAGS[name], 0, direct_from - SOON))
            steps.append((stage_6, name, LAGS["up"] - EAGER, direct_from - SOON, direct_from))
        else:
            steps.append((normal[name], name, LAGS[name], 0, direct_from))
    for number, stage in ((0, direct_0), (1, direct_1), (2, direct_2), (3, direct_3)):
        steps.append((stage, f"d{number}", DLAG[number], direct_from, tasks))

    for matrix in range(matrices):
        own_piece(matrix).start()
    fetches = [pltpu.make_async_copy(f_hbm, features, in_sem.at[0]), pltpu.make_async_copy(b_hbm, bias, in_sem.at[2])] + [
        pltpu.make_async_copy(f_hbm.at[pl.ds(chunk * rows, rows), :], carried.at[chunk], in_sem.at[1])
        for chunk in range(CHUNKS)
    ]
    start(fetches)
    with jax.named_scope("barrier"):
        pl.semaphore_wait(barrier, 8)
    with jax.named_scope("fetch"):
        for matrix in range(matrices):
            own_piece(matrix).wait()
    with jax.named_scope("v0"):
        down_0()
    with jax.named_scope("v0c"):
        for fetch in fetches:
            fetch.wait()

    def weights_at(i, number):
        turn = i - WLAG[number]
        first = turn == WFIRST
        matrix = jnp.where(first, 1, turn // 4 + 2)
        regular = jnp.logical_and(jnp.logical_and(turn >= 0, lax.rem(turn, 4) == 0), matrix < matrices)

        @pl.when(jnp.logical_or(first, regular))
        def _():
            with jax.named_scope(f"w{number}"):
                weight_stages[number](matrix)

    @pl.loop(0, max(direct_from - SOON + LAGS["up"], direct_from + LAGS["up"] - EAGER, tasks + DLAG[3]))
    def _(i):
        weights_at(i, 3)
        for stage, name, lag, first, end in steps:
            t = i - lag

            @pl.when(jnp.logical_and(t >= first, t < end))
            def _(stage=stage, name=name, t=t):
                with jax.named_scope(name):
                    stage(t)

        for number in range(3):
            weights_at(i, number)

    with jax.named_scope("end"):
        sent = (
            near_b, far_b, near_b, far_b, near_a, far_a, near_a, far_a, across_b, across_a, across_a
        )
        for number, size in enumerate(sent):
            send(size, size, ss.at[number], rs.at[0, 0], right).wait_send()
        for number, size in enumerate((from_d, across_d, from_d)):
            send(size, size, sd.at[number], rd.at[0, 0], right).wait_send()
        for matrix in range(matrices):
            place = w_full.at[matrix, pl.ds(0, weight_sends * share), :]
            send(place, place, wss, wrs.at[0, 0], right).wait_send()


def local(features, v_weight, u_weight, cross_bias):
    layers, depth, share = v_weight.shape
    rank = share * lax.axis_size("dp")
    rows = features.shape[0] // CHUNKS
    late = rows - EARLY
    quarter = rank // 4
    tasks = layers * CHUNKS - DIRECT
    dma = pltpu.SemaphoreType.DMA
    anywhere = pl.BlockSpec(memory_space=pltpu.HBM)
    arguments = [
        pltpu.with_memory_space_constraint(array, pltpu.HBM)
        for array in (features, jnp.swapaxes(v_weight, 1, 2), u_weight, cross_bias)
    ]
    return pl.pallas_call(
        kernel,
        out_shape=jax.ShapeDtypeStruct(features.shape, BF16),
        in_specs=[anywhere] * 4,
        out_specs=pl.BlockSpec(memory_space=pltpu.VMEM),
        scratch_shapes=[
            pltpu.VMEM(features.shape, BF16),
            pltpu.VMEM((2 * layers, rank, depth), BF16),
            pltpu.VMEM((CHUNKS, rows, depth), BF16),
            pltpu.VMEM(cross_bias.shape, F32),
            pltpu.VMEM((tasks, 4, late, quarter), BF16),
            pltpu.VMEM((tasks, late, quarter), BF16),
            pltpu.VMEM((tasks, late, quarter), BF16),
            pltpu.VMEM((tasks, 2, late, quarter), BF16),
            pltpu.VMEM((tasks, late, quarter), BF16),
            pltpu.VMEM((tasks, late, quarter), BF16),
            pltpu.VMEM((tasks, 4, late, quarter), BF16),
            pltpu.VMEM((tasks, 2, 4, EARLY, quarter // 2), BF16),
            pltpu.VMEM((tasks, 4, EARLY, quarter // 2), BF16),
            pltpu.VMEM((tasks, 4, EARLY, quarter // 2), BF16),
            pltpu.VMEM((tasks, EARLY, quarter // 2), BF16),
            pltpu.VMEM((tasks, 2, EARLY, quarter // 2), BF16),
            pltpu.VMEM((tasks, 2, 4, EARLY, quarter // 2), BF16),
            pltpu.VMEM((DIRECT, 4, rows, quarter), BF16),
            pltpu.VMEM((DIRECT, 3, rows, quarter), BF16),
            pltpu.VMEM((DIRECT, rows, quarter), BF16),
            pltpu.VMEM((DIRECT, rows, quarter), BF16),
            pltpu.VMEM((DIRECT, 4, rows, quarter), BF16),
            dma((11,)),
            dma((SLOTS, 11)),
            dma,
            dma((2 * layers, 5)),
            dma((3, PARTS)),
            dma((3,)),
            dma((2 * layers,)),
            dma((3,)),
            dma((DIRECT, 3)),
        ],
        compiler_params=pltpu.CompilerParams(
            collective_id=0, has_side_effects=True, vmem_limit_bytes=50 << 20
        ),
    )(*arguments)


def solution(mesh):
    return jax.shard_map(
        local,
        mesh=mesh,
        in_specs=(P("dp", "mp"), P(None, "mp", "dp"), P(None, "dp", "mp"), P(None, "mp")),
        out_specs=P("dp", "mp"),
        check_vma=False,
    )
```

```python
import jax
import jax.numpy as jnp
from jax import lax
from jax.experimental import pallas as pl
from jax.experimental.pallas import tpu as pltpu
from jax.sharding import PartitionSpec as P

MESH = pl.DeviceIdType.MESH
BF16 = jnp.bfloat16
F32 = jnp.float32

CHUNKS = 8
LAGS = {"a1": 2, "a2": 3, "a3": 4, "a4": 5, "b1": 1, "b2": 2, "b3": 3, "b4": 5, "up": 7}
ORDER = ("down", "a1", "a2", "b1", "b2", "a3", "b3", "a4", "b4", "up")
WLAG = (0, 3, 5, 8)
WFIRST = -1
EARLY = 64
UPPER_A, UPPER_B = 32, 32
SLOTS = 8
PARTS = 4
DIRECT = 2
SOON = 1
EAGER = 0
DLAG = (0, 2, 3, 5)


def kernel(
    f_hbm, v_hbm, u_hbm, b_hbm, out_ref,
    features, w_full, carried, bias,
    part_b, far_b, mid_b, near_b, sum_b, across_b, rank_b,
    part_a, across_a, sum_a, far_a, near_a, rank_a,
    part_d, from_d, sum_d, across_d, rank_d,
    ss, rs, wss, wrs, v0s, in_sem, own_sem, sd, rd,
):
    layers = v_hbm.shape[0]
    matrices = 2 * layers
    rows = f_hbm.shape[0] // CHUNKS
    late = rows - EARLY
    depth = f_hbm.shape[1]
    share = u_hbm.shape[1]
    block_width = 2 * share
    tasks = layers * CHUNKS
    quarter = w_full.shape[1] // 4

    dp, mp = lax.axis_index("dp"), lax.axis_index("mp")
    y_hi, z, core = dp // 8, lax.rem(dp // 2, 4), lax.rem(dp, 2)
    y_lo, x = mp // 4, lax.rem(mp, 4)
    xr, xl, xo = lax.rem(x + 1, 4), lax.rem(x + 3, 4), lax.rem(x + 2, 4)
    zr, zl, zo = lax.rem(z + 1, 4), lax.rem(z + 3, 4), lax.rem(z + 2, 4)

    def at(y_hi=y_hi, z=z, core=core, y_lo=y_lo, x=x):
        return ((y_hi * 4 + z) * 2 + core, y_lo * 4 + x)

    right, left, opposite, across = at(x=xr), at(x=xl), at(x=xo), at(y_lo=1 - y_lo)
    z_right, z_left, y_far, partner = at(z=zr), at(z=zl), at(y_hi=1 - y_hi), at(core=1 - core)

    barrier = pltpu.get_barrier_semaphore()
    for device in (right, left, opposite, across, z_right, z_left, y_far, partner):
        pl.semaphore_signal(barrier, inc=1, device_id=device, device_id_type=MESH)

    def send(src, dst, send_sem, recv_sem, device):
        return pltpu.make_async_remote_copy(
            src_ref=src, dst_ref=dst, send_sem=send_sem, recv_sem=recv_sem,
            device_id=device, device_id_type=MESH,
        )

    def start(copies):
        for copy in copies:
            copy.start()

    own, same, other = y_hi * 4 + z, y_hi * 4, (1 - y_hi) * 4

    def piece(matrix, block):
        first = pl.multiple_of(block * block_width + core * share, share)
        return w_full.at[matrix, pl.ds(first, share), :]

    def move(matrix, block, number, device):
        place = piece(matrix, block)
        return send(place, place, wss, wrs.at[matrix, number], device)

    def arrived(matrix, number, pieces):
        place = w_full.at[matrix, pl.ds(0, pieces * share), :]
        send(place, place, wss, wrs.at[matrix, number], partner).wait_recv()

    def own_piece(matrix):
        source = v_hbm if matrix % 2 == 0 else u_hbm
        return pltpu.make_async_copy(source.at[matrix // 2], piece(matrix, own), own_sem.at[matrix])

    def weights_0(matrix):
        start([move(matrix, own, 1, z_right), move(matrix, own, 1, z_left), move(matrix, own, 4, partner)])
        arrived(matrix, 0, 1)
        start([move(matrix, other + z, 2, z_right), move(matrix, other + z, 2, z_left),
               move(matrix, other + z, 4, partner)])

    def weights_1(matrix):
        arrived(matrix, 1, 2)
        start([move(matrix, same + zl, 3, z_right), move(matrix, same + zl, 4, partner),
               move(matrix, same + zr, 4, partner)])
        arrived(matrix, 2, 2)
        start([move(matrix, other + zr, 3, z_left), move(matrix, other + zl, 4, partner),
               move(matrix, other + zr, 4, partner)])

    def weights_2(matrix):
        arrived(matrix, 3, 2)
        start([move(matrix, same + zo, 4, partner), move(matrix, other + zo, 4, partner)])

    def weights_3(matrix):
        arrived(matrix, 4, 8)

    weight_stages = (weights_0, weights_1, weights_2, weights_3)
    weight_sends = 4 + 6 + 3 + 2

    def down_0():
        step = share // PARTS

        def sub(block, s, sem, device):
            first = pl.multiple_of(block * block_width + core * share + s * step, step)
            place = w_full.at[0, pl.ds(first, step), :]
            return send(place, place, wss, sem, device)

        def landed(kind, s):
            sub(own, s, v0s.at[kind, s], partner).wait_recv()

        for s in range(PARTS):
            start([sub(own, s, v0s.at[0, s], z_right), sub(own, s, wrs.at[0, 0], z_left), sub(own, s, v0s.at[1, s], y_far)])
        move(0, own, 4, partner).start()
        for matrix in range(1, matrices):
            move(matrix, own, 0, y_far).start()
        for s in range(PARTS):
            landed(0, s)
            sub(same + zl, s, wrs.at[0, 2], z_right).start()
            landed(1, s)
            start([sub(other + z, s, wrs.at[0, 1], z_right), sub(other + z, s, v0s.at[2, s], z_left)])
        start([move(0, same + zl, 4, partner), move(0, other + z, 4, partner)])
        arrived(0, 0, 1)
        move(0, same + zr, 4, partner).start()
        for s in range(PARTS):
            landed(2, s)
            sub(other + zr, s, wrs.at[0, 3], z_left).start()
        move(0, other + zr, 4, partner).start()
        arrived(0, 1, 1)
        move(0, other + zl, 4, partner).start()
        weights_0(1)
        arrived(0, 2, 1)
        move(0, same + zo, 4, partner).start()
        arrived(0, 3, 1)
        move(0, other + zo, 4, partner).start()
        arrived(0, 4, 8)

    def to_right_and_left(t, rows, upper, part, far, mid, near, rank, first):
        upper, lower = pl.ds(0, upper), pl.ds(upper, rows - upper)

        def hop_1():
            start([
                send(part(xo).at[upper], far.at[t, upper], ss.at[first], rs.at[lax.rem(t, SLOTS), first], right),
                send(part(xo).at[lower], far.at[t, lower], ss.at[first], rs.at[lax.rem(t, SLOTS), first], left),
                send(part(xr).at[lower], near.at[t, 0, lower], ss.at[first], rs.at[lax.rem(t, SLOTS), first + 1], right),
                send(part(xl).at[upper], near.at[t, 0, upper], ss.at[first], rs.at[lax.rem(t, SLOTS), first + 1], left),
            ])

        def hop_2():
            await_recv(t, first, far)
            mid[t, upper] = (part(xr)[upper].astype(F32) + far[t, upper].astype(F32)).astype(BF16)
            mid[t, lower] = (part(xl)[lower].astype(F32) + far[t, lower].astype(F32)).astype(BF16)
            start([
                send(mid.at[t, upper], near.at[t, 1, upper], ss.at[first + 1], rs.at[lax.rem(t, SLOTS), first + 1], right),
                send(mid.at[t, lower], near.at[t, 1, lower], ss.at[first + 1], rs.at[lax.rem(t, SLOTS), first + 1], left),
            ])

        def total():
            await_recv(t, first + 1, near)
            return (
                part(x)[...].astype(F32) + near[t, 0].astype(F32) + near[t, 1].astype(F32)
            ).astype(BF16)

        def share_1():
            start([
                send(rank(x), rank(x), ss.at[first + 2], rs.at[lax.rem(t, SLOTS), first + 2], right),
                send(rank(x), rank(x), ss.at[first + 2], rs.at[lax.rem(t, SLOTS), first + 2], left),
            ])

        def share_2():
            await_recv(t, first + 2, near)
            start([
                send(rank(xl).at[lower], rank(xl).at[lower], ss.at[first + 3], rs.at[lax.rem(t, SLOTS), first + 3], right),
                send(rank(xr).at[upper], rank(xr).at[upper], ss.at[first + 3], rs.at[lax.rem(t, SLOTS), first + 3], left),
            ])

        return hop_1, hop_2, total, share_1, share_2

    def straight(t, part, far, near, rank, first):
        def hop():
            start([
                send(part(xo), far.at[t], ss.at[first + 1], rs.at[lax.rem(t, SLOTS), first], opposite),
                send(part(xr), near.at[t, 0], ss.at[first], rs.at[lax.rem(t, SLOTS), first + 1], right),
                send(part(xl), near.at[t, 1], ss.at[first], rs.at[lax.rem(t, SLOTS), first + 1], left),
            ])

        def total():
            await_recv(t, first, far)
            await_recv(t, first + 1, near)
            return (
                part(x)[...].astype(F32) + near[t, 0].astype(F32) + near[t, 1].astype(F32) + far[t].astype(F32)
            ).astype(BF16)

        upper, lower = pl.ds(0, UPPER_A), pl.ds(UPPER_A, EARLY - UPPER_A)

        def share_1():
            start([
                send(rank(x), rank(x), ss.at[first + 2], rs.at[lax.rem(t, SLOTS), first + 2], right),
                send(rank(x), rank(x), ss.at[first + 2], rs.at[lax.rem(t, SLOTS), first + 2], left),
            ])

        def share_2():
            await_recv(t, first + 2, near)
            for q, part_of, device in ((xl, lower, right), (xr, upper, left)):
                place = rank(q).at[part_of]
                send(place, place, ss.at[first + 3], rs.at[lax.rem(t, SLOTS), first + 3], device).start()

        return hop, total, share_1, share_2

    def ways(t):
        late_ways = to_right_and_left(
            t, late, UPPER_B, lambda q: part_b.at[t, q], far_b, mid_b, near_b, lambda q: rank_b.at[t, q], 0
        )
        early_ways = straight(t, lambda q: sum_a.at[t, q], far_a, near_a, lambda q: rank_a.at[t, y_lo, q], 4)
        return late_ways, early_ways

    def over_y(t, src, dst, number):
        send(src, dst, ss.at[number], rs.at[lax.rem(t, SLOTS), number], across).start()

    def await_recv(t, number, size):
        send(size.at[t], size.at[t], ss.at[0], rs.at[lax.rem(t, SLOTS), number], right).wait_recv()

    def chunk_rows(chunk):
        return pl.ds(pl.multiple_of(chunk * rows, rows), rows)

    def down(t):
        layer, chunk = t // CHUNKS, lax.rem(t, CHUNKS)
        for q in range(4):
            yield q, lax.dot_general(
                carried[chunk],
                w_full[2 * layer, q * quarter : (q + 1) * quarter, :],
                (((1,), (1,)), ((), ())),
                preferred_element_type=F32,
            ).astype(BF16)

    def up(t, lhs):
        layer, chunk = t // CHUNKS, lax.rem(t, CHUNKS)
        for j in range(4):
            columns = slice(j * depth // 4, (j + 1) * depth // 4)
            total = bias[pl.ds(layer, 1), columns]
            for q in range(4):
                total = total + jnp.dot(
                    lhs[q],
                    w_full[2 * layer + 1, q * quarter : (q + 1) * quarter, columns],
                    preferred_element_type=F32,
                )
            carried[chunk, :, columns] = (
                features[chunk_rows(chunk), columns].astype(F32) * total + carried[chunk, :, columns].astype(F32)
            ).astype(BF16)

        @pl.when(layer == layers - 1)
        def _():
            out_ref[chunk_rows(chunk), :] = carried[chunk]

    def stage_0(t):
        for q, value in down(t):
            part_b[t, q] = value[:late]
            part_a[t, 0, q] = value[late:, : quarter // 2]
            part_a[t, 1, q] = value[late:, quarter // 2 :]
        over_y(t, part_a.at[t, 1 - y_lo], across_a.at[t], 9)
        ways(t)[0][0]()

    def early_1(t):
        await_recv(t, 9, across_a)
        sum_a[t] = (part_a[t, y_lo].astype(F32) + across_a[t].astype(F32)).astype(BF16)
        ways(t)[1][0]()

    def early_2(t):
        early_ways = ways(t)[1]
        rank_a[t, y_lo, x] = early_ways[1]()
        early_ways[2]()

    def early_3(t):
        ways(t)[1][3]()

    def early_4(t):
        await_recv(t, 7, far_a)
        over_y(t, rank_a.at[t, y_lo], rank_a.at[t, y_lo], 10)

    def late_1(t):
        ways(t)[0][1]()

    def late_2(t):
        sum_b[t] = ways(t)[0][2]()
        over_y(t, sum_b.at[t], across_b.at[t], 8)

    def late_3(t):
        await_recv(t, 8, across_b)
        rank_b[t, x] = (sum_b[t].astype(F32) + across_b[t].astype(F32)).astype(BF16)
        ways(t)[0][3]()

    def late_4(t):
        ways(t)[0][4]()

    def stage_6(t):
        await_recv(t, 3, far_b)
        await_recv(t, 10, across_a)
        up(t, [
            jnp.concatenate(
                [rank_b[t, q], jnp.concatenate([rank_a[t, 0, q], rank_a[t, 1, q]], axis=1)], axis=0
            )
            for q in range(4)
        ])

    def await_direct(n, number, size):
        send(size, size, sd.at[0], rd.at[n, number], right).wait_recv()

    def direct_0(t):
        n = t - direct_from
        for q, value in down(t):
            part_d[n, q] = value
        start([
            send(part_d.at[n, xo], from_d.at[n, 2], sd.at[0], rd.at[n, 0], opposite),
            send(part_d.at[n, xr], from_d.at[n, 0], sd.at[0], rd.at[n, 0], right),
            send(part_d.at[n, xl], from_d.at[n, 1], sd.at[0], rd.at[n, 0], left),
        ])

    def direct_1(t):
        n = t - direct_from
        await_direct(n, 0, from_d.at[n])
        sum_d[n] = (
            part_d[n, x].astype(F32)
            + from_d[n, 0].astype(F32)
            + from_d[n, 1].astype(F32)
            + from_d[n, 2].astype(F32)
        ).astype(BF16)
        send(sum_d.at[n], across_d.at[n], sd.at[1], rd.at[n, 1], across).start()

    def direct_2(t):
        n = t - direct_from
        await_direct(n, 1, across_d.at[n])
        rank_d[n, x] = (sum_d[n].astype(F32) + across_d[n].astype(F32)).astype(BF16)
        start([
            send(rank_d.at[n, x], rank_d.at[n, x], sd.at[2], rd.at[n, 2], device)
            for device in (opposite, right, left)
        ])

    def direct_3(t):
        n = t - direct_from
        await_direct(n, 2, from_d.at[n])
        up(t, [rank_d[n, q] for q in range(4)])

    direct_from = tasks - DIRECT
    normal = {
        "a1": early_1, "a2": early_2, "a3": early_3, "a4": early_4,
        "b1": late_1, "b2": late_2, "b3": late_3, "b4": late_4, "up": stage_6,
    }
    steps = []
    for name in ORDER:
        if name == "down":
            steps.append((stage_0, name, 0, 0, direct_from))
        elif name == "up":
            steps.append((stage_6, name, LAGS[name], 0, direct_from - SOON))
            steps.append((stage_6, name, LAGS["up"] - EAGER, direct_from - SOON, direct_from))
        else:
            steps.append((normal[name], name, LAGS[name], 0, direct_from))
    for number, stage in ((0, direct_0), (1, direct_1), (2, direct_2), (3, direct_3)):
        steps.append((stage, f"d{number}", DLAG[number], direct_from, tasks))

    for matrix in range(matrices):
        own_piece(matrix).start()
    fetches = [pltpu.make_async_copy(f_hbm, features, in_sem.at[0]), pltpu.make_async_copy(b_hbm, bias, in_sem.at[2])] + [
        pltpu.make_async_copy(f_hbm.at[pl.ds(chunk * rows, rows), :], carried.at[chunk], in_sem.at[1])
        for chunk in range(CHUNKS)
    ]
    start(fetches)
    with jax.named_scope("barrier"):
        pl.semaphore_wait(barrier, 8)
    with jax.named_scope("fetch"):
        for matrix in range(matrices):
            own_piece(matrix).wait()
    with jax.named_scope("v0"):
        down_0()
    with jax.named_scope("v0c"):
        for fetch in fetches:
            fetch.wait()

    def weights_at(i, number):
        turn = i - WLAG[number]
        first = turn == WFIRST
        matrix = jnp.where(first, 1, turn // 4 + 2)
        regular = jnp.logical_and(jnp.logical_and(turn >= 0, lax.rem(turn, 4) == 0), matrix < matrices)

        @pl.when(jnp.logical_or(first, regular))
        def _():
            with jax.named_scope(f"w{number}"):
                weight_stages[number](matrix)

    @pl.loop(0, max(direct_from - SOON + LAGS["up"], direct_from + LAGS["up"] - EAGER, tasks + DLAG[3]))
    def _(i):
        weights_at(i, 3)
        for stage, name, lag, first, end in steps:
            t = i - lag

            @pl.when(jnp.logical_and(t >= first, t < end))
            def _(stage=stage, name=name, t=t):
                with jax.named_scope(name):
                    stage(t)

        for number in range(3):
            weights_at(i, number)

    with jax.named_scope("end"):
        sent = (
            near_b, far_b, near_b, far_b, near_a, far_a, near_a, far_a, across_b, across_a, across_a
        )
        for number, size in enumerate(sent):
            send(size, size, ss.at[number], rs.at[0, 0], right).wait_send()
        for number, size in enumerate((from_d, across_d, from_d)):
            send(size, size, sd.at[number], rd.at[0, 0], right).wait_send()
        for matrix in range(matrices):
            place = w_full.at[matrix, pl.ds(0, weight_sends * share), :]
            send(place, place, wss, wrs.at[0, 0], right).wait_send()


def local(features, v_weight, u_weight, cross_bias):
    layers, depth, share = v_weight.shape
    rank = share * lax.axis_size("dp")
    rows = features.shape[0] // CHUNKS
    late = rows - EARLY
    quarter = rank // 4
    tasks = layers * CHUNKS - DIRECT
    dma = pltpu.SemaphoreType.DMA
    anywhere = pl.BlockSpec(memory_space=pltpu.HBM)
    arguments = [
        pltpu.with_memory_space_constraint(array, pltpu.HBM)
        for array in (features, jnp.swapaxes(v_weight, 1, 2), u_weight, cross_bias)
    ]
    return pl.pallas_call(
        kernel,
        out_shape=jax.ShapeDtypeStruct(features.shape, BF16),
        in_specs=[anywhere] * 4,
        out_specs=pl.BlockSpec(memory_space=pltpu.VMEM),
        scratch_shapes=[
            pltpu.VMEM(features.shape, BF16),
            pltpu.VMEM((2 * layers, rank, depth), BF16),
            pltpu.VMEM((CHUNKS, rows, depth), BF16),
            pltpu.VMEM(cross_bias.shape, F32),
            pltpu.VMEM((tasks, 4, late, quarter), BF16),
            pltpu.VMEM((tasks, late, quarter), BF16),
            pltpu.VMEM((tasks, late, quarter), BF16),
            pltpu.VMEM((tasks, 2, late, quarter), BF16),
            pltpu.VMEM((tasks, late, quarter), BF16),
            pltpu.VMEM((tasks, late, quarter), BF16),
            pltpu.VMEM((tasks, 4, late, quarter), BF16),
            pltpu.VMEM((tasks, 2, 4, EARLY, quarter // 2), BF16),
            pltpu.VMEM((tasks, 4, EARLY, quarter // 2), BF16),
            pltpu.VMEM((tasks, 4, EARLY, quarter // 2), BF16),
            pltpu.VMEM((tasks, EARLY, quarter // 2), BF16),
            pltpu.VMEM((tasks, 2, EARLY, quarter // 2), BF16),
            pltpu.VMEM((tasks, 2, 4, EARLY, quarter // 2), BF16),
            pltpu.VMEM((DIRECT, 4, rows, quarter), BF16),
            pltpu.VMEM((DIRECT, 3, rows, quarter), BF16),
            pltpu.VMEM((DIRECT, rows, quarter), BF16),
            pltpu.VMEM((DIRECT, rows, quarter), BF16),
            pltpu.VMEM((DIRECT, 4, rows, quarter), BF16),
            dma((11,)),
            dma((SLOTS, 11)),
            dma,
            dma((2 * layers, 5)),
            dma((3, PARTS)),
            dma((3,)),
            dma((2 * layers,)),
            dma((3,)),
            dma((DIRECT, 3)),
        ],
        compiler_params=pltpu.CompilerParams(
            collective_id=0, has_side_effects=True, vmem_limit_bytes=50 << 20
        ),
    )(*arguments)


def solution(mesh):
    return jax.shard_map(
        local,
        mesh=mesh,
        in_specs=(P("dp", "mp"), P(None, "mp", "dp"), P(None, "dp", "mp"), P(None, "mp")),
        out_specs=P("dp", "mp"),
        check_vma=False,
    )
```
